256 devices in a mesh: space: 8 (over z_hi, y), inner: 32 (over z_lo, x, core).
Axes of the slice: x: 4, y: 4, z: 8 (z_hi: 2, z_lo: 4; z = z_hi * 4 + z_lo), core: 2. Of those that a mesh axis runs over, the one named last changes fastest.
Arguments:
- hamiltonian: bfloat16 [512, 5, 128, 128], P(('space', 'inner')), as said below
- pattern: int32 [512, 5], P(('space', 'inner')), may hold values from 0 to 1, as said below
- ortho: bfloat16 [512, 2, 128, 128], P(('space', 'inner')), may hold values from -0.25 to 0.25
- lists: int32 [512, 6], P(('space', 'inner')), may hold values from -1 to 511, as said below
Outputs:
- density: float32 [512, 13, 128, 128], P(('space', 'inner'))
The draws below stay inside these ranges and needn't reach their ends.
Inputs may be any that keep to these rules, and one draw needn't show every extreme that they name: Symmetric block band: hamiltonian[j, r] is the transpose of hamiltonian[j + r - 2, 4 - r]; blocks that point outside the matrix are zero. symmetric: pattern[j, r] equals pattern[j + r - 2, 4 - r]; the middle entry is 1; entries that point outside the matrix are 0. lists[j, 0] = j; the next entries are distinct block columns within 5 of j other than j, followed only by -1; each row has 3 to 6 entries that are not -1, and some row has 6.
All inputs are finite; a program needn't handle non-finite values.
Results may differ from the reference program's by a relative error of at most 0.0055.
Values may be sent and summed in bfloat16 or wider, within the bound.
No kernel may reach another device: no remote copies, remote signals or barrier semaphores. Data moves between devices by JAX's collectives and lax.ppermute only.
A program may use at most 64 MiB of HBM per device.

```python
import math
import jax
import jax.numpy as jnp
import numpy as np
from jax import lax

BS = 128
RH = 2
RO = 3
Q = 5
KMAX = 6
KMIN = 3
STEPS = 3
NB = 512


def draw_hamiltonian(key, part):
    band_width = 2 * RH + 1
    raw_values = jax.random.normal(key, (NB, band_width, BS, BS), jnp.float32)
    raw_values = raw_values / math.sqrt(band_width * BS)
    col_index = jnp.arange(NB)[:, None]
    band_index = jnp.arange(band_width)[None, :]
    row_index = col_index + band_index - RH
    inside = (row_index >= 0) & (row_index < NB)
    partner = raw_values[jnp.clip(row_index, 0, NB - 1), 2 * RH - band_index]
    symmetric = 0.5 * (raw_values + jnp.swapaxes(partner, -1, -2))
    return jnp.where(inside[:, :, None, None], symmetric, 0.0).astype(jnp.bfloat16)


def draw_pattern(key, part):
    band_width = 2 * RH + 1
    key = jax.random.fold_in(key, 11)
    marks = (jax.random.randint(key, (NB, band_width), 0, 10) < 7).astype(jnp.int32)
    col_index = jnp.arange(NB)[:, None]
    band_index = jnp.arange(band_width)[None, :]
    row_index = col_index + band_index - RH
    inside = (row_index >= 0) & (row_index < NB)
    partner = marks[jnp.clip(row_index, 0, NB - 1), 2 * RH - band_index]
    joined = jnp.maximum(marks, partner)
    joined = jnp.where(band_index == RH, 1, joined)
    return jnp.where(inside, joined, 0).astype(jnp.int32)


def draw_lists(key, part):
    key = jax.random.fold_in(key, 23)
    first_key, second_key = jax.random.split(key)
    candidates = jnp.concatenate([jnp.arange(-Q, 0), jnp.arange(1, Q + 1)])
    col_index = jnp.arange(NB)
    targets = col_index[:, None] + candidates[None, :]
    inside = (targets >= 0) & (targets < NB)
    scores = jax.random.randint(first_key, (NB, 2 * Q), 0, 1 << 20) * (2 * Q) + jnp.arange(2 * Q)[None, :]
    scores = scores + jnp.where(inside, 0, 1 << 26)
    ranking = jnp.argsort(scores, axis=1)
    chosen = jnp.take_along_axis(targets, ranking, 1)[:, :KMAX - 1]
    counts = jax.random.randint(second_key, (NB,), KMIN, KMAX + 1)
    counts = jnp.where(col_index == NB // 2, KMAX, counts)
    slot_index = jnp.arange(KMAX - 1)[None, :]
    others = jnp.where(slot_index < counts[:, None] - 1, chosen, -1)
    return jnp.concatenate([col_index[:, None], others], 1).astype(jnp.int32)


def steps_of(rng, dims, cuts, low, top_value):
    loudness, own = 1.0, jax.random.fold_in(rng, 6)
    for axis_at, blocks in cuts:
        draws = jnp.exp(jax.random.uniform(jax.random.fold_in(own, axis_at), (blocks,), jnp.float32, low / len(cuts), top_value / len(cuts)))
        loudness = loudness * jnp.repeat(draws, dims[axis_at] // blocks).reshape([-1 if axis == axis_at else 1 for axis in range(len(dims))])
    return loudness


def noise(key, extent, scale, bound, cuts=(), kind=jnp.bfloat16):
    entries = scale * jax.random.normal(key, extent, jnp.float32)
    if cuts:
        entries = entries * steps_of(key, extent, cuts, -0.22, 0.18)
    return jnp.clip(entries, -bound, bound).astype(kind)


def setup_inputs(seed: int = 0) -> dict:
    splits = jax.random.split(jax.random.key(seed), 5)
    hamiltonian = draw_hamiltonian(jax.random.fold_in(splits[4], 71), 0)
    pattern = draw_pattern(jax.random.fold_in(splits[4], 71), 0)
    ortho = noise(splits[2], (NB, 2, BS, BS), (4 * BS) ** -0.5, 0.25, ((0, 256),))
    lists = draw_lists(jax.random.fold_in(splits[4], 71), 0)
    return dict(hamiltonian=hamiltonian, pattern=pattern, ortho=ortho, lists=lists)


chem_level = 0.25

def orth_columns(ham_ext, ortho_ext, ham_off, ortho_off, count):
    column_range = np.arange(count)
    previous = ham_ext[ham_off + column_range - 1].astype(jnp.float32)
    current = ham_ext[ham_off + column_range].astype(jnp.float32)
    upper = ortho_ext[ortho_off + column_range, 0].astype(jnp.float32)
    diagonal = ortho_ext[ortho_off + column_range, 1].astype(jnp.float32)
    row_index = ortho_off + column_range[:, None] + np.arange(-RO, RO + 1)[None, :]
    z_rows = ortho_ext[row_index].astype(jnp.float32)
    left_padded = jnp.pad(previous, ((0, 0), (1, 2), (0, 0), (0, 0)))
    right_padded = jnp.pad(current, ((0, 0), (2, 1), (0, 0), (0, 0)))
    product = jnp.einsum('cgab,cbd->cgad', left_padded, upper, precision=lax.Precision.HIGHEST)
    product = product + jnp.einsum('cgab,cbd->cgad', right_padded, diagonal, precision=lax.Precision.HIGHEST)
    product = lax.optimization_barrier(product.astype(jnp.bfloat16)).astype(jnp.float32)
    result = jnp.einsum('cqba,cqbd->cqad', z_rows[:, :, 0], product[:, :-1], precision=lax.Precision.HIGHEST)
    result = result + jnp.einsum('cqba,cqbd->cqad', z_rows[:, :, 1], product[:, 1:], precision=lax.Precision.HIGHEST)
    return result.astype(jnp.bfloat16)

def mat_product(left, right):
    return jnp.dot(left.astype(jnp.float32), right.astype(jnp.float32), precision=lax.Precision.HIGHEST)

def solve_column(orth_ext, base, slots, column):
    slots = slots.astype(jnp.int32)
    positions = jnp.clip(slots - base, 0, orth_ext.shape[0] - 1).astype(jnp.int32)
    gathered = orth_ext[positions].astype(jnp.float32)
    first_row = 2 * RO + 1 - gathered.shape[1]
    live = slots >= 0
    both_live = live[:, None, None] & live[None, :, None]
    offsets_grid = slots[:, None] - slots[None, :] + RO
    band_rows = jnp.arange(first_row, 2 * RO + 1, dtype=jnp.int32)[None, None, :]
    lower_sel = (offsets_grid[:, :, None] == band_rows) & (offsets_grid >= RO)[:, :, None] & both_live
    upper_sel = ((2 * RO - offsets_grid)[:, :, None] == band_rows) & (offsets_grid < RO)[:, :, None] & both_live
    sub_block = jnp.einsum('str,trab->satb', lower_sel.astype(jnp.float32), gathered, precision=lax.Precision.HIGHEST)
    sub_block = sub_block + jnp.einsum('str,srba->satb', upper_sel.astype(jnp.float32), gathered, precision=lax.Precision.HIGHEST)
    slot_count = gathered.shape[0]
    block_size = gathered.shape[-1]
    order_n = slot_count * block_size
    sub_block = sub_block.reshape(order_n, order_n)
    diag_values = jnp.repeat(live.astype(jnp.float32), block_size)
    shifted = chem_level * jnp.diag(diag_values) - sub_block
    squares = jnp.sum(shifted * shifted)
    live_rows = jnp.sum(live.astype(jnp.float32)) * block_size
    scale = 2.0 * jnp.sqrt(squares / live_rows + 1e-06)
    iterate = (shifted / scale).astype(jnp.bfloat16)
    identity = jnp.eye(order_n, dtype=jnp.float32)
    for step_index in range(STEPS - 1):
        square = mat_product(iterate, iterate)
        factor = (1.5 * identity - 0.5 * square).astype(jnp.bfloat16)
        iterate = mat_product(iterate, factor).astype(jnp.bfloat16)
    columns = iterate[:, :block_size]
    unit = identity[:, :block_size]
    square_col = mat_product(iterate, columns)
    factor_col = (1.5 * unit - 0.5 * square_col).astype(jnp.bfloat16)
    result = mat_product(iterate, factor_col)
    pcol = (0.5 * (unit + result)).reshape(slot_count, block_size, block_size)
    placing = (((slots - column + Q)[:, None] == jnp.arange(2 * Q + 1, dtype=jnp.int32)[None, :]) & live[:, None]).astype(jnp.float32)
    return jnp.einsum('sr,sab->rab', placing, pcol, precision=lax.Precision.HIGHEST)

def back_transform(porth, porth_next, ortho_ext, ortho_off, count):
    column_range = np.arange(count)
    diag_own = ortho_ext[ortho_off + column_range, 1].astype(jnp.float32)
    upper_next = ortho_ext[ortho_off + column_range + 1, 0].astype(jnp.float32)
    low_band = jnp.pad(porth, ((0, 0), (0, 1), (0, 0), (0, 0)))
    high_band = jnp.pad(porth_next, ((0, 0), (1, 0), (0, 0), (0, 0)))
    right_part = jnp.einsum('crab,cdb->crad', low_band, diag_own, precision=lax.Precision.HIGHEST)
    right_part = right_part + jnp.einsum('crab,cdb->crad', high_band, upper_next, precision=lax.Precision.HIGHEST)
    row_index = ortho_off + column_range[:, None] + np.arange(-Q - 1, Q + 2)[None, :]
    diag_rows = ortho_ext[row_index, 1].astype(jnp.float32)
    upper_rows = ortho_ext[row_index + 1, 0].astype(jnp.float32)
    lower_y = jnp.pad(right_part, ((0, 0), (1, 0), (0, 0), (0, 0)))
    upper_y = jnp.pad(right_part, ((0, 0), (0, 1), (0, 0), (0, 0)))
    result = jnp.einsum('cpab,cpbd->cpad', diag_rows, lower_y, precision=lax.Precision.HIGHEST)
    return result + jnp.einsum('cpab,cpbd->cpad', upper_rows, upper_y, precision=lax.Precision.HIGHEST)

def reference(hamiltonian, pattern, ortho, lists):
    total = hamiltonian.shape[0]
    block_size = hamiltonian.shape[-1]
    masked = hamiltonian * pattern[:, :, None, None].astype(jnp.bfloat16)
    index_all = jnp.arange(total, dtype=jnp.int32)
    upper = jnp.where((index_all == 0)[:, None, None], jnp.zeros_like(ortho[:, 0]), ortho[:, 0])
    diag_z = (jnp.eye(block_size, dtype=jnp.float32) + ortho[:, 1].astype(jnp.float32)).astype(jnp.bfloat16)
    stacked = jnp.stack([upper, diag_z], 1)
    margin = Q + RO + 2
    ortho_ext = jnp.pad(stacked, ((margin, margin), (0, 0), (0, 0), (0, 0)))
    ham_ext = jnp.pad(masked, ((1, 0), (0, 0), (0, 0), (0, 0)))
    ham_orth = orth_columns(ham_ext, ortho_ext, 1, margin, total)
    orth_ext = jnp.pad(ham_orth, ((Q, Q), (0, 0), (0, 0), (0, 0)))
    bands = lax.map(lambda item: solve_column(orth_ext, -Q, item[0], item[1]), (lists, index_all))
    following = jnp.concatenate([bands[1:], jnp.zeros_like(bands[:1])], 0)
    return back_transform(bands, following, ortho_ext, margin, total)
```

```python
import functools

import jax
import jax.numpy as jnp
from jax import lax
from jax.experimental import pallas as pl
from jax.experimental.pallas import tpu as pltpu
from jax.sharding import PartitionSpec as P


AXES = ("space", "inner")
BS = 128
RO = 3
KMAX = 6
STEPS = 3
CHEM = 0.25
OWN = 2
SPAN = 14
BACK = 6
ORDER = KMAX * BS
PAY = 10 * BS + 16
FAR = 8 * BS
TILE = 256


BF = jnp.bfloat16
F32 = jnp.float32


def nn(a, b):
    return jnp.dot(a, b, preferred_element_type=F32)


def nt(a, b):
    return lax.dot_general(a, b, (((1,), (1,)), ((), ())), preferred_element_type=F32)


def rows(i, n=1):
    return slice(i * BS, (i + n) * BS)


def eye(n, m):
    r = lax.broadcasted_iota(jnp.int32, (n, m), 0)
    c = lax.broadcasted_iota(jnp.int32, (n, m), 1)
    return jnp.where(r == c, 1.0, 0.0).astype(F32)


def pack_kernel(meta, pattern, lists, ham, ortho, pay, far):
    first, core = meta[0], meta[1]
    for c in range(OWN):
        for r in range(3):
            keep = pattern[c, r + 2].astype(F32)
            block = (ham[c, r + 2].astype(F32) * keep).astype(BF)
            pay[rows(c * 3 + r), :] = block
            far[rows(c * 3 + r), :] = block
        upper = ortho[c, 0]
        if c == 0:
            upper = jnp.where(first == 0, jnp.zeros_like(upper), upper)
        pay[rows(6 + 2 * c), :] = upper
        pay[rows(7 + 2 * c), :] = ortho[c, 1]
    far[rows(6, 2), :] = pay[rows(8, 2), :]

    @pl.when(core == 0)
    def _():
        far[rows(2), :] = pay[rows(6), :]
        far[rows(4), :] = pay[rows(7), :]

    lane = lax.broadcasted_iota(jnp.int32, (16, BS), 1)
    code = jnp.zeros((16, BS), F32)
    for s in range(KMAX):
        slot = lists[0, s]
        value = jnp.where(slot >= 0, slot - first + 8, 0).astype(F32)
        code = code + jnp.where(lane == s, value, 0.0)
    pay[10 * BS : 10 * BS + 16, :] = code.astype(BF)


def main_kernel(
    meta, lists, own, pair, near_a, near_b, cross_a, cross_b, far, out,
    hl, zc, zl, gt, up, xs, ms, ys, pb, rt, slots,
):
    core, odd_chip = meta[1], meta[2]
    ident = eye(BS, BS)

    def take(k, pay, is_far=None):
        i = 2 * k + BACK
        if is_far is None:
            for c in range(OWN):
                hl[i + c] = pay[rows(3 * c, 3), :]
                put_z(i + c, pay[rows(6 + 2 * c), :], pay[rows(7 + 2 * c), :])
        elif is_far == "left":
            for c in range(OWN):
                hl[i + c] = pay[rows(3 * c, 3), :]
            put_z(i + 1, pay[rows(6), :], pay[rows(7), :])
        else:
            for c in range(OWN):
                hl[i + c] = pay[rows(3 * c, 3), :]
            put_z(i, pay[rows(2), :], pay[rows(4), :])
            put_z(i + 1, pay[rows(6), :], pay[rows(7), :])

    def put_z(i, upper, diagonal):
        diag = (ident + diagonal.astype(F32)).astype(BF)
        zc[i, :BS, :] = upper
        zc[i, BS:, :] = diag
        zl[i, :, BS:] = upper
        zl[i + 1, :, :BS] = diag

    def slots_of(pay):
        code = pay[10 * BS : 10 * BS + 16, :].astype(F32)
        lane = lax.broadcasted_iota(jnp.int32, (16, BS), 1)
        row = lax.broadcasted_iota(jnp.int32, (16, BS), 0)
        for s in range(KMAX):
            value = jnp.sum(jnp.where((lane == s) & (row == 0), code, 0.0)).astype(jnp.int32)
            slots[2 * KMAX + s] = jnp.where(value > 0, value - 8 + BACK + 2, -1)

    take(0, own)
    for c in range(OWN):
        for s in range(KMAX):
            slot = lists[c, s]
            slots[c * KMAX + s] = jnp.where(slot >= 0, slot - meta[0] + BACK, -1)

    def sides(near_l, cross_l, near_r, cross_r):
        @pl.when(core == 0)
        def _():
            take(-3, far, "left")
            take(-2, near_l)
            take(-1, cross_l)
            take(1, pair)
            take(2, near_r)
            take(3, cross_r)
            slots_of(pair)

        @pl.when(core == 1)
        def _():
            take(-3, cross_l)
            take(-2, near_l)
            take(-1, pair)
            take(1, cross_r)
            take(2, near_r)
            take(3, far, "right")
            slots_of(cross_r)

    @pl.when(odd_chip == 0)
    def _():
        sides(near_b, cross_b, near_a, cross_a)

    @pl.when(odd_chip == 1)
    def _():
        sides(near_a, cross_a, near_b, cross_b)

    for b in range(1, SPAN):
        zu_t = zc[b, :BS, :].T
        zd_t = zc[b, BS:, :].T
        left = nt(zu_t, hl[b - 1])
        right = nt(zd_t, hl[b])
        edge = nn(zd_t, hl[b - 1, rows(1), :])
        gt[b, :, rows(0)] = (left[:, rows(0)] + edge).astype(BF)
        gt[b, :, rows(1)] = (left[:, rows(1)] + right[:, rows(0)]).astype(BF)
        gt[b, :, rows(2)] = (left[:, rows(2)] + right[:, rows(1)]).astype(BF)
        gt[b, :, rows(3)] = right[:, rows(2)].astype(BF)
    for b in range(1, SPAN):
        for k in range(RO + 1):
            if b + k < SPAN:
                if k < RO:
                    block = nn(gt[b, :, rows(k, 2)], zc[b + k])
                else:
                    block = nn(gt[b, :, rows(k)], zc[b + k, :BS, :])
                up[4 * b + k] = block.astype(BF)

    pb[...] = jnp.zeros_like(pb)

    def solve(c, carry):
        where_to = [slots[c * KMAX + s] for s in range(KMAX)]
        live = [w >= 0 for w in where_to]
        count = functools.reduce(lambda a, b: a + b, [v.astype(jnp.int32) for v in live])
        squares = jnp.zeros((BS, BS), F32)

        def pair_of(s, t):
            ws, wt = where_to[s], where_to[t]
            lo, hi = jnp.minimum(ws, wt), jnp.maximum(ws, wt)
            valid = live[s] & live[t] & (hi - lo <= RO)
            index = jnp.where(valid, 4 * lo + (hi - lo), 0)
            return valid, index, ws >= wt

        for s in range(KMAX):
            block = up[jnp.where(live[s], 4 * where_to[s], 0)].astype(F32)
            entry = jnp.where(live[s], CHEM * ident - block, 0.0)
            squares = squares + entry * entry
            for t in range(s):
                valid, index, _ = pair_of(s, t)
                block = up[index].astype(F32)
                squares = squares + jnp.where(valid, 2.0 * (block * block), 0.0)
        total = jnp.sum(squares, axis=(0, 1), keepdims=True)
        width = (jnp.maximum(count, 1) * BS).astype(F32)
        scale = 2.0 * jnp.sqrt(total / width + 1e-06)
        inverse = 1.0 / scale
        for s in range(KMAX):
            block = up[jnp.where(live[s], 4 * where_to[s], 0)].astype(F32)
            entry = jnp.where(live[s], CHEM * ident - block, 0.0) * inverse
            xs[rows(s), rows(s)] = entry.astype(BF)
            for t in range(s):
                valid, index, below = pair_of(s, t)
                block = jnp.where(valid, up[index].astype(F32) * -inverse, 0.0).astype(BF)
                turned = block.T
                xs[rows(s), rows(t)] = jnp.where(below, turned, block)
                xs[rows(t), rows(s)] = jnp.where(below, block, turned)

        tiles = [slice(i * TILE, (i + 1) * TILE) for i in range(ORDER // TILE)]
        big = eye(TILE, TILE)
        src, dst = xs, ys
        for _ in range(STEPS - 1):
            for m in tiles:
                for n in tiles:
                    square = nn(src[m, :], src[:, n])
                    base = 1.5 * big if m == n else 0.0
                    ms[m, n] = (base - 0.5 * square).astype(BF)
            for m in tiles:
                for n in tiles:
                    dst[m, n] = nn(src[m, :], ms[:, n]).astype(BF)
            src, dst = dst, src
        top = eye(TILE, BS)
        for m in tiles:
            square = nn(src[m, :], src[:, :BS])
            base = 1.5 * top if m.start == 0 else 0.0
            ms[m, :BS] = (base - 0.5 * square).astype(BF)
        lanes = pl.ds(pl.multiple_of(c * BS, BS), BS)
        for i, m in enumerate(tiles):
            part = nn(src[m, :], ms[:, :BS])
            if i == 0:
                part = part + top
            part = (0.5 * part).astype(BF)
            for h in range(TILE // BS):
                s = i * (TILE // BS) + h
                row = jnp.where(live[s], where_to[s], SPAN)
                pb[pl.ds(pl.multiple_of(row * BS, BS), BS), lanes] = part[rows(h), :]
        return carry

    lax.fori_loop(0, OWN + 1, solve, 0)

    for c in range(OWN):
        rt[:, rows(c)] = nt(pb[BS : SPAN * BS, rows(c, 2)], zl[BACK + c + 1]).astype(BF)
    for i in range(SPAN):
        if i == 0:
            part = nn(zl[1, :, BS:], rt[rows(0), :])
        elif i == SPAN - 1:
            part = nn(zl[i + 1, :, :BS], rt[rows(i - 1), :])
        else:
            part = nn(zl[i + 1], rt[rows(i - 1, 2), :])
        for c in range(OWN):
            if 0 <= i - c < 13:
                out[c, i - c] = part[:, rows(c)]


def build(mesh, interpret=False):
    n = mesh.shape["space"] * mesh.shape["inner"]
    inside = lambda i: 0 <= i < n
    swap = [(i, i ^ 1) for i in range(n)]

    def chips(parity):
        pairs = []
        for i in range(n):
            chip = i >> 1
            other = chip + 1 if (chip & 1) == parity else chip - 1
            pairs.append((i, 2 * other + (i & 1)))
        return [(a, b) for a, b in pairs if inside(b)]

    cross = [(i, i + 3 if i & 1 else i - 3) for i in range(n)]
    cross = [(a, b) for a, b in cross if inside(b)]

    def send(value, pairs):
        return lax.ppermute(value, AXES, pairs)

    vmem = pl.BlockSpec(memory_space=pltpu.VMEM)
    smem = pl.BlockSpec(memory_space=pltpu.SMEM)

    def local(hamiltonian, pattern, ortho, lists):
        device = lax.axis_index(AXES).astype(jnp.int32)
        meta = jnp.stack([device * OWN, device & 1, (device >> 1) & 1, device])
        pay, far = pl.pallas_call(
            pack_kernel,
            out_shape=(
                jax.ShapeDtypeStruct((PAY, BS), BF),
                jax.ShapeDtypeStruct((FAR, BS), BF),
            ),
            in_specs=[smem, smem, smem, vmem, vmem],
            out_specs=(vmem, vmem),
            compiler_params=pltpu.CompilerParams(vmem_limit_bytes=8 << 20),
            interpret=interpret,
        )(meta, pattern, lists, hamiltonian, ortho)
        near_b = send(pay, chips(1))
        near_a = send(pay, chips(0))
        got_far = send(far, cross)
        pair = send(pay, swap)
        cross_a = send(near_a, swap)
        cross_b = send(near_b, swap)
        out = pl.pallas_call(
            main_kernel,
            out_shape=jax.ShapeDtypeStruct((OWN, 13, BS, BS), F32),
            in_specs=[smem, smem] + [vmem] * 7,
            out_specs=vmem,
            scratch_shapes=[
                pltpu.VMEM((SPAN, 3 * BS, BS), BF),
                pltpu.VMEM((SPAN, 2 * BS, BS), BF),
                pltpu.VMEM((SPAN + 1, BS, 2 * BS), BF),
                pltpu.VMEM((SPAN, BS, 4 * BS), BF),
                pltpu.VMEM((4 * SPAN, BS, BS), BF),
                pltpu.VMEM((ORDER, ORDER), BF),
                pltpu.VMEM((ORDER, ORDER), BF),
                pltpu.VMEM((ORDER, ORDER), BF),
                pltpu.VMEM(((SPAN + 1) * BS, 3 * BS), BF),
                pltpu.VMEM(((SPAN - 1) * BS, 2 * BS), BF),
                pltpu.SMEM((3 * KMAX,), jnp.int32),
            ],
            compiler_params=pltpu.CompilerParams(vmem_limit_bytes=24 << 20),
            cost_estimate=pl.CostEstimate(
                flops=12 * 10**9, bytes_accessed=4 << 20, transcendentals=0
            ),
            interpret=interpret,
        )(meta, lists, pay, pair, near_a, near_b, cross_a, cross_b, got_far)
        return out

    spec4 = P(AXES, None, None, None)
    spec2 = P(AXES, None)
    return jax.shard_map(
        local, mesh=mesh, in_specs=(spec4, spec2, spec4, spec2), out_specs=spec4, check_vma=False
    )


def solution(mesh):
    return build(mesh)
```

```python
import functools

import jax
import jax.numpy as jnp
from jax import lax
from jax.experimental import pallas as pl
from jax.experimental.pallas import tpu as pltpu
from jax.sharding import PartitionSpec as P


AXES = ("space", "inner")
BS = 128
RO = 3
KMAX = 6
STEPS = 3
CHEM = 0.25
OWN = 2
SPAN = 14
BACK = 6
ORDER = KMAX * BS
PAY = 9 * BS + 16
FAR = 7 * BS + 16
LISTS = 9
TILE = 256


BF = jnp.bfloat16
F32 = jnp.float32


def nn(a, b):
    return jnp.dot(a, b, preferred_element_type=F32)


def nt(a, b):
    return lax.dot_general(a, b, (((1,), (1,)), ((), ())), preferred_element_type=F32)


def rows(i, n=1):
    return slice(i * BS, (i + n) * BS)


def eye(n, m):
    r = lax.broadcasted_iota(jnp.int32, (n, m), 0)
    c = lax.broadcasted_iota(jnp.int32, (n, m), 1)
    return jnp.where(r == c, 1.0, 0.0).astype(F32)


def pack_kernel(meta, ham, ortho, pay, far, hs, os, sems):
    first, core = meta[0], meta[1]
    copies = [
        pltpu.make_async_copy(ham.at[c, pl.ds(2, 3)], hs.at[c], sems.at[c]) for c in range(OWN)
    ] + [pltpu.make_async_copy(ortho, os, sems.at[OWN])]
    for copy in copies:
        copy.start()
    for copy in copies:
        copy.wait()

    r = lax.broadcasted_iota(jnp.int32, (BS, BS), 0)
    c = lax.broadcasted_iota(jnp.int32, (BS, BS), 1)
    masked = [
        [hs[j, k].astype(F32) * meta[3 + 3 * j + k].astype(F32) for k in range(3)]
        for j in range(OWN)
    ]
    pay[rows(0), :] = jnp.where(r >= c, masked[0][0], masked[1][0]).astype(BF)
    for j in range(OWN):
        for k in range(1, 3):
            pay[rows(2 * j + k), :] = masked[j][k].astype(BF)
    pay[rows(5), :] = os[1, 0]
    pay[rows(6), :] = os[1, 1]
    pay[rows(7), :] = (os[0, 0].astype(F32) * jnp.where(first == 0, 0.0, 1.0)).astype(BF)
    pay[rows(8), :] = os[0, 1]
    diagonal = jnp.sum(jnp.where(r == c, masked[1][0], 0.0), axis=0, keepdims=True)
    lane = lax.broadcasted_iota(jnp.int32, (16, BS), 1)
    row = lax.broadcasted_iota(jnp.int32, (16, BS), 0)
    extra = jnp.where(row == 1, diagonal, 0.0)
    for s in range(KMAX):
        slot = meta[LISTS + s]
        value = jnp.where(slot >= 0, slot + 2, 0).astype(F32)
        extra = extra + jnp.where((lane == s) & (row == 0), value, 0.0)
    pay[PAY - 16 : PAY, :] = extra.astype(BF)

    far[rows(0, 7), :] = pay[rows(0, 7), :]
    far[FAR - 16 : FAR, :] = extra.astype(BF)

    @pl.when(core == 0)
    def _():
        far[rows(2, 2), :] = pay[rows(7, 2), :]


def main_kernel(
    meta, own, pair, near_a, near_b, cross_a, cross_b, far, out,
    hl, zc, zl, gt, up, xs, ms, ys, pb, rt, ob, slots, sems,
):
    core, odd_chip = meta[1], meta[2]
    r = lax.broadcasted_iota(jnp.int32, (BS, BS), 0)
    c = lax.broadcasted_iota(jnp.int32, (BS, BS), 1)
    ident = eye(BS, BS)

    def put_z(i, upper, diagonal):
        diag = (ident + diagonal.astype(F32)).astype(BF)
        zc[i, :BS, :] = upper
        zc[i, BS:, :] = diag
        zl[i, :, BS:] = upper
        zl[i + 1, :, :BS] = diag

    def take(k, pay, from_far=None):
        i = 2 * k + BACK
        size = PAY if from_far is None else FAR
        both = pay[rows(0), :].astype(F32)
        turned = pay[rows(0), :].T.astype(F32)
        last = pay[size - 16 : size, :].astype(F32)[1:2, :]
        hl[i, rows(0), :] = jnp.where(r >= c, both, turned).astype(BF)
        hl[i + 1, rows(0), :] = jnp.where(
            r < c, both, jnp.where(r > c, turned, jnp.broadcast_to(last, (BS, BS)))
        ).astype(BF)
        hl[i, rows(1, 2), :] = pay[rows(1, 2), :]
        hl[i + 1, rows(1, 2), :] = pay[rows(3, 2), :]
        put_z(i + 1, pay[rows(5), :], pay[rows(6), :])
        if from_far is None:
            put_z(i, pay[rows(7), :], pay[rows(8), :])
        elif from_far == "right":
            put_z(i, pay[rows(2), :], pay[rows(3), :])

    def slots_of(pay):
        code = pay[PAY - 16 : PAY, :].astype(F32)
        lane = lax.broadcasted_iota(jnp.int32, (16, BS), 1)
        row = lax.broadcasted_iota(jnp.int32, (16, BS), 0)
        for s in range(KMAX):
            value = jnp.sum(jnp.where((lane == s) & (row == 0), code, 0.0)).astype(jnp.int32)
            slots[2 * KMAX + s] = jnp.where(value > 0, value, -1)

    take(0, own)
    for s in range(OWN * KMAX):
        slots[s] = meta[LISTS + s]

    def sides(near_l, cross_l, near_r, cross_r):
        @pl.when(core == 0)
        def _():
            take(-3, far, "left")
            take(-2, near_l)
            take(-1, cross_l)
            take(1, pair)
            take(2, near_r)
            take(3, cross_r)
            slots_of(pair)

        @pl.when(core == 1)
        def _():
            take(-3, cross_l)
            take(-2, near_l)
            take(-1, pair)
            take(1, cross_r)
            take(2, near_r)
            take(3, far, "right")
            slots_of(cross_r)

    @pl.when(odd_chip == 0)
    def _():
        sides(near_b, cross_b, near_a, cross_a)

    @pl.when(odd_chip == 1)
    def _():
        sides(near_a, cross_a, near_b, cross_b)

    for b in range(1, SPAN):
        zu_t = zc[b, :BS, :].T
        zd_t = zc[b, BS:, :].T
        left = nt(zu_t, hl[b - 1])
        right = nt(zd_t, hl[b])
        edge = nn(zd_t, hl[b - 1, rows(1), :])
        gt[b, :, rows(0)] = (left[:, rows(0)] + edge).astype(BF)
        gt[b, :, rows(1)] = (left[:, rows(1)] + right[:, rows(0)]).astype(BF)
        gt[b, :, rows(2)] = (left[:, rows(2)] + right[:, rows(1)]).astype(BF)
        gt[b, :, rows(3)] = right[:, rows(2)].astype(BF)
    for b in range(1, SPAN):
        for k in range(RO + 1):
            if b + k < SPAN:
                if k < RO:
                    block = nn(gt[b, :, rows(k, 2)], zc[b + k])
                else:
                    block = nn(gt[b, :, rows(k)], zc[b + k, :BS, :])
                up[4 * b + k] = (-block).astype(BF)

    pb[...] = jnp.zeros_like(pb)

    def solve(c, carry):
        where_to = [slots[c * KMAX + s] for s in range(KMAX)]
        live = [w >= 0 for w in where_to]
        count = functools.reduce(lambda a, b: a + b, [v.astype(jnp.int32) for v in live])
        squares = jnp.zeros((BS, BS), F32)
        for s in range(KMAX):
            block = up[jnp.where(live[s], 4 * where_to[s], 0)].astype(F32)
            entry = jnp.where(live[s], CHEM * ident + block, 0.0)
            squares = squares + entry * entry
            xs[rows(s), rows(s)] = entry.astype(BF)
            for t in range(s):
                ws, wt = where_to[s], where_to[t]
                lo, hi = jnp.minimum(ws, wt), jnp.maximum(ws, wt)
                valid = live[s] & live[t] & (hi - lo <= RO)
                block = up[jnp.where(valid, 4 * lo + (hi - lo), 0)]
                turned = block.T
                block = jnp.where(valid, block, jnp.zeros_like(block))
                turned = jnp.where(valid, turned, jnp.zeros_like(turned))
                xs[rows(s), rows(t)] = jnp.where(ws >= wt, turned, block)
                xs[rows(t), rows(s)] = jnp.where(ws >= wt, block, turned)
                wide = block.astype(F32)
                squares = squares + 2.0 * (wide * wide)
        total = jnp.sum(squares, axis=(0, 1), keepdims=True)
        width = (jnp.maximum(count, 1) * BS).astype(F32)
        inverse = 1.0 / (2.0 * jnp.sqrt(total / width + 1e-06))
        half = 0.5 * inverse * inverse

        tiles = [slice(i * TILE, (i + 1) * TILE) for i in range(ORDER // TILE)]
        big = eye(TILE, TILE)
        src, dst = xs, ys
        for step in range(STEPS - 1):
            for i, m in enumerate(tiles):
                for n in tiles[: i + 1]:
                    square = nn(src[m, :], src[:, n])
                    base = 1.5 * big if m == n else 0.0
                    ms[m, n] = (base - (half if step == 0 else 0.5) * square).astype(BF)
            for i, m in enumerate(tiles):
                for n in tiles[: i + 1]:
                    value = nn(src[m, n.start :], ms[n.start :, n])
                    if n.start:
                        value = value + nt(src[m, : n.start], ms[n, : n.start])
                    if step == 0:
                        value = value * inverse
                    value = value.astype(BF)
                    dst[m, n] = value
                    if m != n:
                        dst[n, m] = value.T
            src, dst = dst, src
        top = eye(TILE, BS)
        for m in tiles:
            square = nn(src[m, :], src[:, :BS])
            base = 1.5 * top if m.start == 0 else 0.0
            ms[m, :BS] = (base - 0.5 * square).astype(BF)
        lanes = pl.ds(pl.multiple_of(c * BS, BS), BS)
        for i, m in enumerate(tiles):
            part = nn(src[m, :], ms[:, :BS])
            if i == 0:
                part = part + top
            part = (0.5 * part).astype(BF)
            for h in range(TILE // BS):
                s = i * (TILE // BS) + h
                row = jnp.where(live[s], where_to[s], SPAN)
                pb[pl.ds(pl.multiple_of(row * BS, BS), BS), lanes] = part[rows(h), :]
        return carry

    lax.fori_loop(0, OWN + 1, solve, 0)

    for j in range(OWN):
        rt[:, rows(j)] = nt(pb[BS : SPAN * BS, rows(j, 2)], zl[BACK + j + 1]).astype(BF)
    copies = []
    for i in range(SPAN):
        if i == 0:
            part = nn(zl[1, :, BS:], rt[rows(0), :])
        elif i == SPAN - 1:
            part = nn(zl[i + 1, :, :BS], rt[rows(i - 1), :])
        else:
            part = nn(zl[i + 1], rt[rows(i - 1, 2), :])
        for j in range(OWN):
            if 0 <= i - j < 13:
                ob[j, i - j] = part[:, rows(j)]
                copy = pltpu.make_async_copy(
                    ob.at[j, i - j], out.at[j, i - j], sems.at[j * 13 + i - j]
                )
                copy.start()
                copies.append(copy)
    for copy in copies:
        copy.wait()


def scratch():
    return [
        pltpu.VMEM((SPAN, 3 * BS, BS), BF),
        pltpu.VMEM((SPAN, 2 * BS, BS), BF),
        pltpu.VMEM((SPAN + 1, BS, 2 * BS), BF),
        pltpu.VMEM((SPAN, BS, 4 * BS), BF),
        pltpu.VMEM((4 * SPAN, BS, BS), BF),
        pltpu.VMEM((ORDER, ORDER), BF),
        pltpu.VMEM((ORDER, ORDER), BF),
        pltpu.VMEM((ORDER, ORDER), BF),
        pltpu.VMEM(((SPAN + 1) * BS, 3 * BS), BF),
        pltpu.VMEM(((SPAN - 1) * BS, 2 * BS), BF),
        pltpu.VMEM((OWN, 13, BS, BS), F32),
        pltpu.SMEM((3 * KMAX,), jnp.int32),
        pltpu.SemaphoreType.DMA((OWN * 13,)),
    ]


def build(mesh, interpret=False):
    n = mesh.shape["space"] * mesh.shape["inner"]
    inside = lambda i: 0 <= i < n
    swap = [(i, i ^ 1) for i in range(n)]

    def chips(parity):
        pairs = []
        for i in range(n):
            chip = i >> 1
            other = chip + 1 if (chip & 1) == parity else chip - 1
            pairs.append((i, 2 * other + (i & 1)))
        return [(a, b) for a, b in pairs if inside(b)]

    cross = [(i, i + 3 if i & 1 else i - 3) for i in range(n)]
    cross = [(a, b) for a, b in cross if inside(b)]

    def send(value, pairs):
        return lax.ppermute(value, AXES, pairs)

    in_hbm = lambda x: x if interpret else pltpu.with_memory_space_constraint(x, pltpu.HBM)
    vmem = pl.BlockSpec(memory_space=pltpu.VMEM)
    smem = pl.BlockSpec(memory_space=pltpu.SMEM)
    anywhere = pl.BlockSpec(memory_space=pltpu.HBM)

    def local(hamiltonian, pattern, ortho, lists):
        device = lax.axis_index(AXES).astype(jnp.int32)
        first = device * OWN
        meta = jnp.concatenate(
            [
                jnp.stack([first, device & 1, (device >> 1) & 1]),
                pattern[:, 2:].reshape(-1),
                jnp.where(lists >= 0, lists - first + BACK, -1).reshape(-1),
            ]
        )
        pay, far = pl.pallas_call(
            pack_kernel,
            out_shape=(jax.ShapeDtypeStruct((PAY, BS), BF), jax.ShapeDtypeStruct((FAR, BS), BF)),
            in_specs=[smem, anywhere, anywhere],
            out_specs=(vmem, vmem),
            scratch_shapes=[
                pltpu.VMEM((OWN, 3, BS, BS), BF),
                pltpu.VMEM((OWN, 2, BS, BS), BF),
                pltpu.SemaphoreType.DMA((OWN + 1,)),
            ],
            compiler_params=pltpu.CompilerParams(vmem_limit_bytes=8 << 20),
            interpret=interpret,
        )(meta, in_hbm(hamiltonian), in_hbm(ortho))
        near_b = send(pay, chips(1))
        near_a = send(pay, chips(0))
        got_far = send(far, cross)
        pair = send(pay, swap)
        cross_a = send(near_a, swap)
        cross_b = send(near_b, swap)
        out = pl.pallas_call(
            main_kernel,
            out_shape=jax.ShapeDtypeStruct((OWN, 13, BS, BS), F32),
            in_specs=[smem] + [vmem] * 7,
            out_specs=anywhere,
            scratch_shapes=scratch(),
            compiler_params=pltpu.CompilerParams(vmem_limit_bytes=24 << 20),
            cost_estimate=pl.CostEstimate(
                flops=12 * 10**9, bytes_accessed=4 << 20, transcendentals=0
            ),
            interpret=interpret,
        )(meta, pay, pair, near_a, near_b, cross_a, cross_b, got_far)
        return out

    spec4 = P(AXES, None, None, None)
    spec2 = P(AXES, None)
    return jax.shard_map(
        local, mesh=mesh, in_specs=(spec4, spec2, spec4, spec2), out_specs=spec4, check_vma=False
    )


def solution(mesh):
    return build(mesh)
```

```python
import functools

import jax
import jax.numpy as jnp
from jax import lax
from jax.experimental import pallas as pl
from jax.experimental.pallas import tpu as pltpu
from jax.sharding import PartitionSpec as P


AXES = ("space", "inner")
BS = 128
RO = 3
KMAX = 6
STEPS = 3
CHEM = 0.25
OWN = 2
SPAN = 14
BACK = 6
ORDER = KMAX * BS
PAY = 9 * BS + 16
FAR = 7 * BS + 16
TILE = 256


BF = jnp.bfloat16
F32 = jnp.float32


def nn(a, b):
    return jnp.dot(a, b, preferred_element_type=F32)


def nt(a, b):
    return lax.dot_general(a, b, (((1,), (1,)), ((), ())), preferred_element_type=F32)


def rows(i, n=1):
    return slice(i * BS, (i + n) * BS)


def eye(n, m):
    r = lax.broadcasted_iota(jnp.int32, (n, m), 0)
    c = lax.broadcasted_iota(jnp.int32, (n, m), 1)
    return jnp.where(r == c, 1.0, 0.0).astype(F32)


def position():
    device = lax.axis_index(AXES).astype(jnp.int32)
    return device * OWN, device & 1, (device >> 1) & 1


def pack_kernel(pattern, lists, ham, ortho, pay, far, keep, slot_of, hs, os, sems):
    first, core, _ = position()
    copies = [
        pltpu.make_async_copy(ham.at[c, pl.ds(2, 3)], hs.at[c], sems.at[c]) for c in range(OWN)
    ] + [
        pltpu.make_async_copy(ortho, os, sems.at[OWN]),
        pltpu.make_async_copy(pattern, keep, sems.at[OWN + 1]),
        pltpu.make_async_copy(lists, slot_of, sems.at[OWN + 2]),
    ]
    for copy in copies:
        copy.start()
    for copy in copies:
        copy.wait()

    r = lax.broadcasted_iota(jnp.int32, (BS, BS), 0)
    c = lax.broadcasted_iota(jnp.int32, (BS, BS), 1)
    masked = [
        [hs[j, k].astype(F32) * keep[j, k + 2].astype(F32) for k in range(3)]
        for j in range(OWN)
    ]
    pay[rows(0), :] = jnp.where(r >= c, masked[0][0], masked[1][0]).astype(BF)
    for j in range(OWN):
        for k in range(1, 3):
            pay[rows(2 * j + k), :] = masked[j][k].astype(BF)
    pay[rows(5), :] = os[1, 0]
    pay[rows(6), :] = os[1, 1]
    pay[rows(7), :] = (os[0, 0].astype(F32) * jnp.where(first == 0, 0.0, 1.0)).astype(BF)
    pay[rows(8), :] = os[0, 1]
    diagonal = jnp.sum(jnp.where(r == c, masked[1][0], 0.0), axis=0, keepdims=True)
    lane = lax.broadcasted_iota(jnp.int32, (16, BS), 1)
    row = lax.broadcasted_iota(jnp.int32, (16, BS), 0)
    extra = jnp.where(row == 1, diagonal, 0.0)
    for s in range(KMAX):
        slot = slot_of[0, s]
        value = jnp.where(slot >= 0, slot - first + BACK + 2, 0).astype(F32)
        extra = extra + jnp.where((lane == s) & (row == 0), value, 0.0)
    pay[PAY - 16 : PAY, :] = extra.astype(BF)

    far[rows(0, 7), :] = pay[rows(0, 7), :]
    far[FAR - 16 : FAR, :] = extra.astype(BF)

    @pl.when(core == 0)
    def _():
        far[rows(2, 2), :] = pay[rows(7, 2), :]


def main_kernel(
    lists, own, pair, near_a, near_b, cross_a, cross_b, far, out,
    hb, zc, zl, gt, up, xs, ms, ys, pb, rt, ob, slots, slot_of, sems,
):
    first, core, odd_chip = position()
    lists_copy = pltpu.make_async_copy(lists, slot_of, sems.at[0])
    lists_copy.start()
    row_at = lax.broadcasted_iota(jnp.int32, (BS, BS), 0)
    lane_at = lax.broadcasted_iota(jnp.int32, (BS, BS), 1)
    ident = eye(BS, BS)

    def put_z(i, upper, diagonal):
        diag = (ident + diagonal.astype(F32)).astype(BF)
        zc[i, :BS, :] = upper
        zc[i, BS:, :] = diag
        zl[i, :, BS:] = upper
        zl[i + 1, :, :BS] = diag

    def put_h(i, k, block):
        hb[i, rows(k + 1), BS:] = block
        if i + 1 < SPAN:
            hb[i + 1, rows(k), :BS] = block
        if k == 1 and i + 1 < SPAN:
            hb[i + 1, rows(0), BS:] = block.T

    def take(k, pay, from_far=None):
        i = 2 * k + BACK
        size = PAY if from_far is None else FAR
        both = pay[rows(0), :].astype(F32)
        turned = pay[rows(0), :].T.astype(F32)
        last = pay[size - 16 : size, :].astype(F32)[1:2, :]
        put_h(i, 0, jnp.where(row_at >= lane_at, both, turned).astype(BF))
        diagonal = jnp.where(
            row_at < lane_at,
            both,
            jnp.where(row_at > lane_at, turned, jnp.broadcast_to(last, (BS, BS))),
        )
        put_h(i + 1, 0, diagonal.astype(BF))
        for j in range(OWN):
            for k in range(1, 3):
                put_h(i + j, k, pay[rows(2 * j + k), :])
        put_z(i + 1, pay[rows(5), :], pay[rows(6), :])
        if from_far is None:
            put_z(i, pay[rows(7), :], pay[rows(8), :])
        elif from_far == "right":
            put_z(i, pay[rows(2), :], pay[rows(3), :])

    def slots_of(pay):
        code = pay[PAY - 16 : PAY, :].astype(F32)
        lane = lax.broadcasted_iota(jnp.int32, (16, BS), 1)
        row = lax.broadcasted_iota(jnp.int32, (16, BS), 0)
        for s in range(KMAX):
            value = jnp.sum(jnp.where((lane == s) & (row == 0), code, 0.0)).astype(jnp.int32)
            slots[2 * KMAX + s] = jnp.where(value > 0, value, -1)

    take(0, own)

    def sides(near_l, cross_l, near_r, cross_r):
        @pl.when(core == 0)
        def _():
            take(-3, far, "left")
            take(-2, near_l)
            take(-1, cross_l)
            take(1, pair)
            take(2, near_r)
            take(3, cross_r)
            slots_of(pair)

        @pl.when(core == 1)
        def _():
            take(-3, cross_l)
            take(-2, near_l)
            take(-1, pair)
            take(1, cross_r)
            take(2, near_r)
            take(3, far, "right")
            slots_of(cross_r)

    @pl.when(odd_chip == 0)
    def _():
        sides(near_b, cross_b, near_a, cross_a)

    @pl.when(odd_chip == 1)
    def _():
        sides(near_a, cross_a, near_b, cross_b)

    for b in range(1, SPAN):
        hb[b, rows(3), :BS] = jnp.zeros((BS, BS), BF)
        gt[b] = nt(zc[b].T, hb[b]).astype(BF)
    for b in range(1, SPAN):
        for k in range(RO + 1):
            if b + k < SPAN:
                if k < RO:
                    block = nn(gt[b, :, rows(k, 2)], zc[b + k])
                else:
                    block = nn(gt[b, :, rows(k)], zc[b + k, :BS, :])
                up[4 * b + k] = (-block).astype(BF)

    lists_copy.wait()
    for j in range(OWN):
        for s in range(KMAX):
            slot = slot_of[j, s]
            slots[j * KMAX + s] = jnp.where(slot >= 0, slot - first + BACK, -1)
    pb[...] = jnp.zeros_like(pb)

    tiles = [slice(i * TILE, (i + 1) * TILE) for i in range(ORDER // TILE)]
    big = eye(TILE, TILE)
    top = eye(TILE, BS)

    def places(c):
        where_to = [slots[c * KMAX + s] for s in range(KMAX)]
        return where_to, [w >= 0 for w in where_to]

    def assemble(c, result):
        where_to, live = places(c)
        count = functools.reduce(lambda a, b: a + b, [v.astype(jnp.int32) for v in live])
        squares = jnp.zeros((BS, BS), F32)
        x = xs.at[c % 2]
        for s in range(KMAX):
            block = up[jnp.where(live[s], 4 * where_to[s], 0)].astype(F32)
            entry = jnp.where(live[s], CHEM * ident + block, 0.0)
            squares = squares + entry * entry
            x[rows(s), rows(s)] = entry.astype(BF)
            yield
            for t in range(s):
                ws, wt = where_to[s], where_to[t]
                lo, hi = jnp.minimum(ws, wt), jnp.maximum(ws, wt)
                valid = live[s] & live[t] & (hi - lo <= RO)
                block = up[jnp.where(valid, 4 * lo + (hi - lo), 0)]
                turned = block.T
                block = jnp.where(valid, block, jnp.zeros_like(block))
                turned = jnp.where(valid, turned, jnp.zeros_like(turned))
                x[rows(s), rows(t)] = jnp.where(ws >= wt, turned, block)
                x[rows(t), rows(s)] = jnp.where(ws >= wt, block, turned)
                wide = block.astype(F32)
                squares = squares + 2.0 * (wide * wide)
                yield
        total = jnp.sum(squares, axis=(0, 1), keepdims=True)
        width = (jnp.maximum(count, 1) * BS).astype(F32)
        inverse = 1.0 / (2.0 * jnp.sqrt(total / width + 1e-06))
        result.extend([inverse, 0.5 * inverse * inverse])

    def solve(c, inverse, half):
        where_to, live = places(c)
        src, dst = xs.at[c % 2], ys
        for step in range(STEPS - 1):
            for i, m in enumerate(tiles):
                for n in tiles[: i + 1]:
                    square = nn(src[m, :], src[:, n])
                    base = 1.5 * big if m == n else 0.0
                    ms[m, n] = (base - (half if step == 0 else 0.5) * square).astype(BF)
                    yield
            for i, m in enumerate(tiles):
                for n in tiles[: i + 1]:
                    value = nn(src[m, n.start :], ms[n.start :, n])
                    if n.start:
                        value = value + nt(src[m, : n.start], ms[n, : n.start])
                    if step == 0:
                        value = value * inverse
                    value = value.astype(BF)
                    dst[m, n] = value
                    if m != n:
                        dst[n, m] = value.T
                    yield
            src, dst = dst, src
        for m in tiles:
            square = nn(src[m, :], src[:, :BS])
            base = 1.5 * top if m.start == 0 else 0.0
            ms[m, :BS] = (base - 0.5 * square).astype(BF)
            yield
        for i, m in enumerate(tiles):
            part = nn(src[m, :], ms[:, :BS])
            if i == 0:
                part = part + top
            part = (0.5 * part).astype(BF)
            for h in range(TILE // BS):
                s = i * (TILE // BS) + h
                row = jnp.where(live[s], where_to[s], SPAN)
                pb[pl.ds(pl.multiple_of(row * BS, BS), BS), rows(c)] = part[rows(h), :]
            yield

    scales = []
    for _ in assemble(0, scales):
        pass
    for c in range(OWN + 1):
        following = []
        coming = assemble(c + 1, following) if c < OWN else iter(())
        for _ in solve(c, *scales):
            next(coming, None)
        for _ in coming:
            pass
        scales = following

    for j in range(OWN):
        rt[:, rows(j)] = nt(pb[BS : SPAN * BS, rows(j, 2)], zl[BACK + j + 1]).astype(BF)
    copies = []
    for i in range(SPAN):
        if i == 0:
            part = nn(zl[1, :, BS:], rt[rows(0), :])
        elif i == SPAN - 1:
            part = nn(zl[i + 1, :, :BS], rt[rows(i - 1), :])
        else:
            part = nn(zl[i + 1], rt[rows(i - 1, 2), :])
        for j in range(OWN):
            if 0 <= i - j < 13:
                ob[j, i - j] = part[:, rows(j)]
                copy = pltpu.make_async_copy(
                    ob.at[j, i - j], out.at[j, i - j], sems.at[j * 13 + i - j]
                )
                copy.start()
                copies.append(copy)
    for copy in copies:
        copy.wait()


def scratch():
    return [
        pltpu.VMEM((SPAN, 4 * BS, 2 * BS), BF),
        pltpu.VMEM((SPAN, 2 * BS, BS), BF),
        pltpu.VMEM((SPAN + 1, BS, 2 * BS), BF),
        pltpu.VMEM((SPAN, BS, 4 * BS), BF),
        pltpu.VMEM((4 * SPAN, BS, BS), BF),
        pltpu.VMEM((2, ORDER, ORDER), BF),
        pltpu.VMEM((ORDER, ORDER), BF),
        pltpu.VMEM((ORDER, ORDER), BF),
        pltpu.VMEM(((SPAN + 1) * BS, 3 * BS), BF),
        pltpu.VMEM(((SPAN - 1) * BS, 2 * BS), BF),
        pltpu.VMEM((OWN, 13, BS, BS), F32),
        pltpu.SMEM((3 * KMAX,), jnp.int32),
        pltpu.SMEM((OWN, KMAX), jnp.int32),
        pltpu.SemaphoreType.DMA((OWN * 13,)),
    ]


def build(mesh, interpret=False):
    n = mesh.shape["space"] * mesh.shape["inner"]
    inside = lambda i: 0 <= i < n
    swap = [(i, i ^ 1) for i in range(n)]

    def chips(parity):
        pairs = []
        for i in range(n):
            chip = i >> 1
            other = chip + 1 if (chip & 1) == parity else chip - 1
            pairs.append((i, 2 * other + (i & 1)))
        return [(a, b) for a, b in pairs if inside(b)]

    cross = [(i, i + 3 if i & 1 else i - 3) for i in range(n)]
    cross = [(a, b) for a, b in cross if inside(b)]

    def send(value, pairs):
        return lax.ppermute(value, AXES, pairs)

    in_hbm = lambda x: x if interpret else pltpu.with_memory_space_constraint(x, pltpu.HBM)
    vmem = pl.BlockSpec(memory_space=pltpu.VMEM)
    anywhere = pl.BlockSpec(memory_space=pltpu.HBM)

    def local(hamiltonian, pattern, ortho, lists):
        pay, far = pl.pallas_call(
            pack_kernel,
            out_shape=(jax.ShapeDtypeStruct((PAY, BS), BF), jax.ShapeDtypeStruct((FAR, BS), BF)),
            in_specs=[anywhere] * 4,
            out_specs=(vmem, vmem),
            scratch_shapes=[
                pltpu.SMEM(pattern.shape, jnp.int32),
                pltpu.SMEM(lists.shape, jnp.int32),
                pltpu.VMEM((OWN, 3, BS, BS), BF),
                pltpu.VMEM((OWN, 2, BS, BS), BF),
                pltpu.SemaphoreType.DMA((OWN + 3,)),
            ],
            compiler_params=pltpu.CompilerParams(vmem_limit_bytes=8 << 20),
            interpret=interpret,
        )(in_hbm(pattern), in_hbm(lists), in_hbm(hamiltonian), in_hbm(ortho))
        near_b = send(pay, chips(1))
        near_a = send(pay, chips(0))
        got_far = send(far, cross)
        pair = send(pay, swap)
        cross_a = send(near_a, swap)
        cross_b = send(near_b, swap)
        out = pl.pallas_call(
            main_kernel,
            out_shape=jax.ShapeDtypeStruct((OWN, 13, BS, BS), F32),
            in_specs=[anywhere] + [vmem] * 7,
            out_specs=anywhere,
            scratch_shapes=scratch(),
            compiler_params=pltpu.CompilerParams(vmem_limit_bytes=24 << 20),
            cost_estimate=pl.CostEstimate(
                flops=12 * 10**9, bytes_accessed=4 << 20, transcendentals=0
            ),
            interpret=interpret,
        )(in_hbm(lists), pay, pair, near_a, near_b, cross_a, cross_b, got_far)
        return out

    spec4 = P(AXES, None, None, None)
    spec2 = P(AXES, None)
    return jax.shard_map(
        local, mesh=mesh, in_specs=(spec4, spec2, spec4, spec2), out_specs=spec4, check_vma=False
    )


def solution(mesh):
    return build(mesh)
```

```python
import functools

import jax
import jax.numpy as jnp
from jax import lax
from jax.experimental import pallas as pl
from jax.experimental.pallas import tpu as pltpu
from jax.sharding import PartitionSpec as P


AXES = ("space", "inner")
BS = 128
RO = 3
KMAX = 6
STEPS = 3
CHEM = 0.25
OWN = 2
SPAN = 14
BACK = 6
ORDER = KMAX * BS
PAY = 9 * BS + 16
FAR = 7 * BS + 16
TILE = 256


BF = jnp.bfloat16
F32 = jnp.float32


def nn(a, b):
    return jnp.dot(a, b, preferred_element_type=F32)


def nt(a, b):
    return lax.dot_general(a, b, (((1,), (1,)), ((), ())), preferred_element_type=F32)


def rows(i, n=1):
    return slice(i * BS, (i + n) * BS)


def eye(n, m):
    r = lax.broadcasted_iota(jnp.int32, (n, m), 0)
    c = lax.broadcasted_iota(jnp.int32, (n, m), 1)
    return jnp.where(r == c, 1.0, 0.0).astype(F32)


def position():
    device = lax.axis_index(AXES).astype(jnp.int32)
    return device * OWN, device & 1, (device >> 1) & 1


def pack_kernel(pattern, lists, ham, ortho, pay, far, keep, slot_of, hs, os, sems):
    first, core, _ = position()
    copies = [
        pltpu.make_async_copy(ham.at[c, pl.ds(2, 3)], hs.at[c], sems.at[c]) for c in range(OWN)
    ] + [
        pltpu.make_async_copy(ortho, os, sems.at[OWN]),
        pltpu.make_async_copy(pattern, keep, sems.at[OWN + 1]),
        pltpu.make_async_copy(lists, slot_of, sems.at[OWN + 2]),
    ]
    for copy in copies:
        copy.start()
    for copy in copies:
        copy.wait()

    r = lax.broadcasted_iota(jnp.int32, (BS, BS), 0)
    c = lax.broadcasted_iota(jnp.int32, (BS, BS), 1)
    masked = [
        [hs[j, k].astype(F32) * keep[j, k + 2].astype(F32) for k in range(3)]
        for j in range(OWN)
    ]
    pay[rows(0), :] = jnp.where(r >= c, masked[0][0], masked[1][0]).astype(BF)
    for j in range(OWN):
        for k in range(1, 3):
            pay[rows(2 * j + k), :] = masked[j][k].astype(BF)
    pay[rows(5), :] = os[1, 0]
    pay[rows(6), :] = os[1, 1]
    pay[rows(7), :] = (os[0, 0].astype(F32) * jnp.where(first == 0, 0.0, 1.0)).astype(BF)
    pay[rows(8), :] = os[0, 1]
    diagonal = jnp.sum(jnp.where(r == c, masked[1][0], 0.0), axis=0, keepdims=True)
    lane = lax.broadcasted_iota(jnp.int32, (16, BS), 1)
    row = lax.broadcasted_iota(jnp.int32, (16, BS), 0)
    extra = jnp.where(row == 1, diagonal, 0.0)
    for s in range(KMAX):
        slot = slot_of[0, s]
        value = jnp.where(slot >= 0, slot - first + BACK + 2, 0).astype(F32)
        extra = extra + jnp.where((lane == s) & (row == 0), value, 0.0)
    pay[PAY - 16 : PAY, :] = extra.astype(BF)

    far[rows(0, 7), :] = pay[rows(0, 7), :]
    far[FAR - 16 : FAR, :] = extra.astype(BF)

    @pl.when(core == 0)
    def _():
        far[rows(2, 2), :] = pay[rows(7, 2), :]


def main_kernel(
    lists, own, pair, near_a, near_b, cross_a, cross_b, far, out,
    hb, zc, zl, gt, up, xs, ms, ys, pb, rt, ob, slots, slot_of, sems,
):
    first, core, odd_chip = position()
    lists_copy = pltpu.make_async_copy(lists, slot_of, sems.at[0])
    lists_copy.start()
    row_at = lax.broadcasted_iota(jnp.int32, (BS, BS), 0)
    lane_at = lax.broadcasted_iota(jnp.int32, (BS, BS), 1)
    ident = eye(BS, BS)

    def put_z(i, upper, diagonal):
        diag = (ident + diagonal.astype(F32)).astype(BF)
        zc[i, :BS, :] = upper
        zc[i, BS:, :] = diag
        zl[i, :, BS:] = upper
        zl[i + 1, :, :BS] = diag

    def put_h(i, k, block):
        hb[i, rows(k + 1), BS:] = block
        if i + 1 < SPAN:
            hb[i + 1, rows(k), :BS] = block
        if k == 1 and i + 1 < SPAN:
            hb[i + 1, rows(0), BS:] = block.T

    def take(k, pay, from_far=None):
        i = 2 * k + BACK
        size = PAY if from_far is None else FAR
        both = pay[rows(0), :].astype(F32)
        turned = pay[rows(0), :].T.astype(F32)
        last = pay[size - 16 : size, :].astype(F32)[1:2, :]
        put_h(i, 0, jnp.where(row_at >= lane_at, both, turned).astype(BF))
        diagonal = jnp.where(
            row_at < lane_at,
            both,
            jnp.where(row_at > lane_at, turned, jnp.broadcast_to(last, (BS, BS))),
        )
        put_h(i + 1, 0, diagonal.astype(BF))
        for j in range(OWN):
            for k in range(1, 3):
                put_h(i + j, k, pay[rows(2 * j + k), :])
        put_z(i + 1, pay[rows(5), :], pay[rows(6), :])
        if from_far is None:
            put_z(i, pay[rows(7), :], pay[rows(8), :])
        elif from_far == "right":
            put_z(i, pay[rows(2), :], pay[rows(3), :])

    def slots_of(pay):
        code = pay[PAY - 16 : PAY, :].astype(F32)
        lane = lax.broadcasted_iota(jnp.int32, (16, BS), 1)
        row = lax.broadcasted_iota(jnp.int32, (16, BS), 0)
        for s in range(KMAX):
            value = jnp.sum(jnp.where((lane == s) & (row == 0), code, 0.0)).astype(jnp.int32)
            slots[2 * KMAX + s] = jnp.where(value > 0, value, -1)

    take(0, own)

    def sides(near_l, cross_l, near_r, cross_r):
        @pl.when(core == 0)
        def _():
            take(-3, far, "left")
            take(-2, near_l)
            take(-1, cross_l)
            take(1, pair)
            take(2, near_r)
            take(3, cross_r)
            slots_of(pair)

        @pl.when(core == 1)
        def _():
            take(-3, cross_l)
            take(-2, near_l)
            take(-1, pair)
            take(1, cross_r)
            take(2, near_r)
            take(3, far, "right")
            slots_of(cross_r)

    @pl.when(odd_chip == 0)
    def _():
        sides(near_b, cross_b, near_a, cross_a)

    @pl.when(odd_chip == 1)
    def _():
        sides(near_a, cross_a, near_b, cross_b)

    for b in range(1, SPAN):
        hb[b, rows(3), :BS] = jnp.zeros((BS, BS), BF)
        gt[b] = nt(zc[b].T, hb[b]).astype(BF)
    for b in range(1, SPAN):
        for k in range(RO + 1):
            if b + k < SPAN:
                if k < RO:
                    block = nn(gt[b, :, rows(k, 2)], zc[b + k])
                else:
                    block = nn(gt[b, :, rows(k)], zc[b + k, :BS, :])
                up[4 * b + k] = (-block).astype(BF)

    lists_copy.wait()
    for j in range(OWN):
        for s in range(KMAX):
            slot = slot_of[j, s]
            slots[j * KMAX + s] = jnp.where(slot >= 0, slot - first + BACK, -1)
    pb[...] = jnp.zeros_like(pb)

    tiles = [slice(i * TILE, (i + 1) * TILE) for i in range(ORDER // TILE)]
    big = eye(TILE, TILE)
    top = eye(BS, ORDER)

    def places(c):
        where_to = [slots[c * KMAX + s] for s in range(KMAX)]
        return where_to, [w >= 0 for w in where_to]

    def assemble(c, result):
        where_to, live = places(c)
        count = functools.reduce(lambda a, b: a + b, [v.astype(jnp.int32) for v in live])
        squares = jnp.zeros((BS, BS), F32)
        x = xs.at[c % 2]
        for s in range(KMAX):
            block = up[jnp.where(live[s], 4 * where_to[s], 0)].astype(F32)
            entry = jnp.where(live[s], CHEM * ident + block, 0.0)
            squares = squares + entry * entry
            x[rows(s), rows(s)] = entry.astype(BF)
            yield
            for t in range(s):
                ws, wt = where_to[s], where_to[t]
                lo, hi = jnp.minimum(ws, wt), jnp.maximum(ws, wt)
                valid = live[s] & live[t] & (hi - lo <= RO)
                block = up[jnp.where(valid, 4 * lo + (hi - lo), 0)]
                turned = block.T
                block = jnp.where(valid, block, jnp.zeros_like(block))
                turned = jnp.where(valid, turned, jnp.zeros_like(turned))
                x[rows(s), rows(t)] = jnp.where(ws >= wt, turned, block)
                x[rows(t), rows(s)] = jnp.where(ws >= wt, block, turned)
                wide = block.astype(F32)
                squares = squares + 2.0 * (wide * wide)
                yield
        total = jnp.sum(squares, axis=(0, 1), keepdims=True)
        width = (jnp.maximum(count, 1) * BS).astype(F32)
        inverse = 1.0 / (2.0 * jnp.sqrt(total / width + 1e-06))
        result.extend([inverse, 0.5 * inverse * inverse])

    def solve(c, inverse, half):
        where_to, live = places(c)
        src, dst = xs.at[c % 2], ys
        for step in range(STEPS - 1):
            for i, m in enumerate(tiles):
                for n in tiles[: i + 1]:
                    square = nn(src[m, :], src[:, n])
                    base = 1.5 * big if m == n else 0.0
                    ms[m, n] = (base - (half if step == 0 else 0.5) * square).astype(BF)
                    yield
            for i, m in enumerate(tiles):
                for n in tiles[: i + 1]:
                    value = nn(src[m, n.start :], ms[n.start :, n])
                    if n.start:
                        value = value + nt(src[m, : n.start], ms[n, : n.start])
                    if step == 0:
                        value = value * inverse
                    value = value.astype(BF)
                    dst[m, n] = value
                    if m != n:
                        dst[n, m] = value.T
                    yield
            src, dst = dst, src
        square = nn(src[:BS, :], src[...])
        ms[:BS, :] = (1.5 * top - 0.5 * square).astype(BF)
        yield
        part = nn(ms[:BS, :], src[...])
        part = (0.5 * (top + part)).astype(BF)
        for s in range(KMAX):
            place = jnp.where(live[s], where_to[s], SPAN)
            pb[rows(c), pl.ds(pl.multiple_of(place * BS, BS), BS)] = part[:, rows(s)]
            yield

    scales = []
    for _ in assemble(0, scales):
        pass
    for c in range(OWN + 1):
        following = []
        coming = assemble(c + 1, following) if c < OWN else iter(())
        for _ in solve(c, *scales):
            next(coming, None)
        for _ in coming:
            pass
        scales = following

    for j in range(OWN):
        rt[rows(j), :] = nn(zl[BACK + j + 1], pb[rows(j, 2), BS : SPAN * BS]).astype(BF)
    copies = []
    for i in range(SPAN):
        if i == 0:
            part = nt(zl[1, :, BS:], rt[:, rows(0)])
        elif i == SPAN - 1:
            part = nt(zl[i + 1, :, :BS], rt[:, rows(i - 1)])
        else:
            part = nt(zl[i + 1], rt[:, rows(i - 1, 2)])
        for j in range(OWN):
            if 0 <= i - j < 13:
                ob[j, i - j] = part[:, rows(j)]
                copy = pltpu.make_async_copy(
                    ob.at[j, i - j], out.at[j, i - j], sems.at[j * 13 + i - j]
                )
                copy.start()
                copies.append(copy)
    for copy in copies:
        copy.wait()


def scratch():
    return [
        pltpu.VMEM((SPAN, 4 * BS, 2 * BS), BF),
        pltpu.VMEM((SPAN, 2 * BS, BS), BF),
        pltpu.VMEM((SPAN + 1, BS, 2 * BS), BF),
        pltpu.VMEM((SPAN, BS, 4 * BS), BF),
        pltpu.VMEM((4 * SPAN, BS, BS), BF),
        pltpu.VMEM((2, ORDER, ORDER), BF),
        pltpu.VMEM((ORDER, ORDER), BF),
        pltpu.VMEM((ORDER, ORDER), BF),
        pltpu.VMEM((3 * BS, (SPAN + 1) * BS), BF),
        pltpu.VMEM((2 * BS, (SPAN - 1) * BS), BF),
        pltpu.VMEM((OWN, 13, BS, BS), F32),
        pltpu.SMEM((3 * KMAX,), jnp.int32),
        pltpu.SMEM((OWN, KMAX), jnp.int32),
        pltpu.SemaphoreType.DMA((OWN * 13,)),
    ]


def build(mesh, interpret=False):
    n = mesh.shape["space"] * mesh.shape["inner"]
    inside = lambda i: 0 <= i < n
    swap = [(i, i ^ 1) for i in range(n)]

    def chips(parity):
        pairs = []
        for i in range(n):
            chip = i >> 1
            other = chip + 1 if (chip & 1) == parity else chip - 1
            pairs.append((i, 2 * other + (i & 1)))
        return [(a, b) for a, b in pairs if inside(b)]

    cross = [(i, i + 3 if i & 1 else i - 3) for i in range(n)]
    cross = [(a, b) for a, b in cross if inside(b)]

    def send(value, pairs):
        return lax.ppermute(value, AXES, pairs)

    in_hbm = lambda x: x if interpret else pltpu.with_memory_space_constraint(x, pltpu.HBM)
    vmem = pl.BlockSpec(memory_space=pltpu.VMEM)
    anywhere = pl.BlockSpec(memory_space=pltpu.HBM)

    def local(hamiltonian, pattern, ortho, lists):
        pay, far = pl.pallas_call(
            pack_kernel,
            out_shape=(jax.ShapeDtypeStruct((PAY, BS), BF), jax.ShapeDtypeStruct((FAR, BS), BF)),
            in_specs=[anywhere] * 4,
            out_specs=(vmem, vmem),
            scratch_shapes=[
                pltpu.SMEM(pattern.shape, jnp.int32),
                pltpu.SMEM(lists.shape, jnp.int32),
                pltpu.VMEM((OWN, 3, BS, BS), BF),
                pltpu.VMEM((OWN, 2, BS, BS), BF),
                pltpu.SemaphoreType.DMA((OWN + 3,)),
            ],
            compiler_params=pltpu.CompilerParams(vmem_limit_bytes=8 << 20),
            interpret=interpret,
        )(in_hbm(pattern), in_hbm(lists), in_hbm(hamiltonian), in_hbm(ortho))
        near_b = send(pay, chips(1))
        near_a = send(pay, chips(0))
        got_far = send(far, cross)
        pair = send(pay, swap)
        cross_a = send(near_a, swap)
        cross_b = send(near_b, swap)
        out = pl.pallas_call(
            main_kernel,
            out_shape=jax.ShapeDtypeStruct((OWN, 13, BS, BS), F32),
            in_specs=[anywhere] + [vmem] * 7,
            out_specs=anywhere,
            scratch_shapes=scratch(),
            compiler_params=pltpu.CompilerParams(vmem_limit_bytes=24 << 20),
            cost_estimate=pl.CostEstimate(
                flops=12 * 10**9, bytes_accessed=4 << 20, transcendentals=0
            ),
            interpret=interpret,
        )(in_hbm(lists), pay, pair, near_a, near_b, cross_a, cross_b, got_far)
        return out

    spec4 = P(AXES, None, None, None)
    spec2 = P(AXES, None)
    return jax.shard_map(
        local, mesh=mesh, in_specs=(spec4, spec2, spec4, spec2), out_specs=spec4, check_vma=False
    )


def solution(mesh):
    return build(mesh)
```

```python
import functools

import jax
import jax.numpy as jnp
from jax import lax
from jax.experimental import pallas as pl
from jax.experimental.pallas import tpu as pltpu
from jax.sharding import PartitionSpec as P


AXES = ("space", "inner")
BS = 128
RO = 3
KMAX = 6
STEPS = 3
CHEM = 0.25
OWN = 2
SPAN = 14
BACK = 6
ORDER = KMAX * BS
PAY = 9 * BS + 16
FAR = 7 * BS + 16
TILE = 256


BF = jnp.bfloat16
F32 = jnp.float32


def nn(a, b):
    return jnp.dot(a, b, preferred_element_type=F32)


def nt(a, b):
    return lax.dot_general(a, b, (((1,), (1,)), ((), ())), preferred_element_type=F32)


def rows(i, n=1):
    return slice(i * BS, (i + n) * BS)


def eye(n, m):
    r = lax.broadcasted_iota(jnp.int32, (n, m), 0)
    c = lax.broadcasted_iota(jnp.int32, (n, m), 1)
    return jnp.where(r == c, 1.0, 0.0).astype(F32)


def position():
    device = lax.axis_index(AXES).astype(jnp.int32)
    return device * OWN, device & 1, (device >> 1) & 1


def pack_kernel(pattern, lists, ham, ortho, pay, far, keep, slot_of, hs, os, sems):
    first, core, _ = position()
    copies = [
        pltpu.make_async_copy(ham.at[c, pl.ds(2, 3)], hs.at[c], sems.at[c]) for c in range(OWN)
    ] + [
        pltpu.make_async_copy(ortho, os, sems.at[OWN]),
        pltpu.make_async_copy(pattern, keep, sems.at[OWN + 1]),
        pltpu.make_async_copy(lists, slot_of, sems.at[OWN + 2]),
    ]
    for copy in copies:
        copy.start()
    for copy in copies:
        copy.wait()

    r = lax.broadcasted_iota(jnp.int32, (BS, BS), 0)
    c = lax.broadcasted_iota(jnp.int32, (BS, BS), 1)
    masked = [
        [hs[j, k].astype(F32) * keep[j, k + 2].astype(F32) for k in range(3)]
        for j in range(OWN)
    ]
    pay[rows(0), :] = jnp.where(r >= c, masked[0][0], masked[1][0]).astype(BF)
    for j in range(OWN):
        for k in range(1, 3):
            pay[rows(2 * j + k), :] = masked[j][k].astype(BF)
    pay[rows(5), :] = os[1, 0]
    pay[rows(6), :] = os[1, 1]
    pay[rows(7), :] = (os[0, 0].astype(F32) * jnp.where(first == 0, 0.0, 1.0)).astype(BF)
    pay[rows(8), :] = os[0, 1]
    diagonal = jnp.sum(jnp.where(r == c, masked[1][0], 0.0), axis=0, keepdims=True)
    lane = lax.broadcasted_iota(jnp.int32, (16, BS), 1)
    row = lax.broadcasted_iota(jnp.int32, (16, BS), 0)
    extra = jnp.where(row == 1, diagonal, 0.0)
    for s in range(KMAX):
        slot = slot_of[0, s]
        value = jnp.where(slot >= 0, slot - first + BACK + 2, 0).astype(F32)
        extra = extra + jnp.where((lane == s) & (row == 0), value, 0.0)
    pay[PAY - 16 : PAY, :] = extra.astype(BF)

    far[rows(0, 7), :] = pay[rows(0, 7), :]
    far[FAR - 16 : FAR, :] = extra.astype(BF)

    @pl.when(core == 0)
    def _():
        far[rows(2, 2), :] = pay[rows(7, 2), :]


def main_kernel(
    lists, own, pair, near_a, near_b, cross_a, cross_b, far, out,
    hb, zc, zl, gt, up, xs, ms, ys, pb, rt, ob, slots, slot_of, sems,
):
    first, core, odd_chip = position()
    lists_copy = pltpu.make_async_copy(lists, slot_of, sems.at[0])
    lists_copy.start()
    row_at = lax.broadcasted_iota(jnp.int32, (BS, BS), 0)
    lane_at = lax.broadcasted_iota(jnp.int32, (BS, BS), 1)
    ident = eye(BS, BS)

    def put_z(i, upper, diagonal):
        diag = (ident + diagonal.astype(F32)).astype(BF)
        zc[i, :BS, :] = upper
        zc[i, BS:, :] = diag
        zl[i, :, BS:] = upper
        zl[i + 1, :, :BS] = diag

    def put_h(i, k, block):
        hb[i, rows(k + 1), BS:] = block
        if i + 1 < SPAN:
            hb[i + 1, rows(k), :BS] = block
        if k == 1 and i + 1 < SPAN:
            hb[i + 1, rows(0), BS:] = block.T

    def take(k, pay, from_far=None):
        i = 2 * k + BACK
        size = PAY if from_far is None else FAR
        both = pay[rows(0), :].astype(F32)
        turned = pay[rows(0), :].T.astype(F32)
        last = pay[size - 16 : size, :].astype(F32)[1:2, :]
        put_h(i, 0, jnp.where(row_at >= lane_at, both, turned).astype(BF))
        diagonal = jnp.where(
            row_at < lane_at,
            both,
            jnp.where(row_at > lane_at, turned, jnp.broadcast_to(last, (BS, BS))),
        )
        put_h(i + 1, 0, diagonal.astype(BF))
        for j in range(OWN):
            for k in range(1, 3):
                put_h(i + j, k, pay[rows(2 * j + k), :])
        put_z(i + 1, pay[rows(5), :], pay[rows(6), :])
        if from_far is None:
            put_z(i, pay[rows(7), :], pay[rows(8), :])
        elif from_far == "right":
            put_z(i, pay[rows(2), :], pay[rows(3), :])

    def slots_of(pay):
        code = pay[PAY - 16 : PAY, :].astype(F32)
        lane = lax.broadcasted_iota(jnp.int32, (16, BS), 1)
        row = lax.broadcasted_iota(jnp.int32, (16, BS), 0)
        for s in range(KMAX):
            value = jnp.sum(jnp.where((lane == s) & (row == 0), code, 0.0)).astype(jnp.int32)
            slots[2 * KMAX + s] = jnp.where(value > 0, value, -1)

    take(0, own)

    def sides(near_l, cross_l, near_r, cross_r):
        @pl.when(core == 0)
        def _():
            take(-3, far, "left")
            take(-2, near_l)
            take(-1, cross_l)
            take(1, pair)
            take(2, near_r)
            take(3, cross_r)
            slots_of(pair)

        @pl.when(core == 1)
        def _():
            take(-3, cross_l)
            take(-2, near_l)
            take(-1, pair)
            take(1, cross_r)
            take(2, near_r)
            take(3, far, "right")
            slots_of(cross_r)

    @pl.when(odd_chip == 0)
    def _():
        sides(near_b, cross_b, near_a, cross_a)

    @pl.when(odd_chip == 1)
    def _():
        sides(near_a, cross_a, near_b, cross_b)

    for b in range(1, SPAN):
        hb[b, rows(3), :BS] = jnp.zeros((BS, BS), BF)
        gt[b] = nt(zc[b].T, hb[b]).astype(BF)
    for b in range(1, SPAN):
        for k in range(RO + 1):
            if b + k < SPAN:
                if k < RO:
                    block = nn(gt[b, :, rows(k, 2)], zc[b + k])
                else:
                    block = nn(gt[b, :, rows(k)], zc[b + k, :BS, :])
                up[4 * b + k] = (-block).astype(BF)

    lists_copy.wait()
    for j in range(OWN):
        for s in range(KMAX):
            slot = slot_of[j, s]
            slots[j * KMAX + s] = jnp.where(slot >= 0, slot - first + BACK, -1)
    pb[...] = jnp.zeros_like(pb)

    tiles = [slice(i * TILE, (i + 1) * TILE) for i in range(ORDER // TILE)]
    big = eye(TILE, TILE)
    top = eye(BS, ORDER)

    def places(c):
        where_to = [slots[c * KMAX + s] for s in range(KMAX)]
        return where_to, [w >= 0 for w in where_to]

    def assemble(c, result):
        where_to, live = places(c)
        count = functools.reduce(lambda a, b: a + b, [v.astype(jnp.int32) for v in live])
        squares = jnp.zeros((BS, BS), F32)
        x = xs.at[c % 2]
        for s in range(KMAX):
            block = up[jnp.where(live[s], 4 * where_to[s], 0)].astype(F32)
            entry = jnp.where(live[s], CHEM * ident + block, 0.0)
            squares = squares + entry * entry
            x[rows(s), rows(s)] = entry.astype(BF)
            yield
            for t in range(s):
                ws, wt = where_to[s], where_to[t]
                lo, hi = jnp.minimum(ws, wt), jnp.maximum(ws, wt)
                valid = live[s] & live[t] & (hi - lo <= RO)
                block = up[jnp.where(valid, 4 * lo + (hi - lo), 0)]
                turned = block.T
                block = jnp.where(valid, block, jnp.zeros_like(block))
                turned = jnp.where(valid, turned, jnp.zeros_like(turned))
                x[rows(s), rows(t)] = jnp.where(ws >= wt, turned, block)
                x[rows(t), rows(s)] = jnp.where(ws >= wt, block, turned)
                wide = block.astype(F32)
                squares = squares + 2.0 * (wide * wide)
                yield
        total = jnp.sum(squares, axis=(0, 1), keepdims=True)
        width = (jnp.maximum(count, 1) * BS).astype(F32)
        inverse = 1.0 / (2.0 * jnp.sqrt(total / width + 1e-06))
        result.extend([inverse, 0.5 * inverse * inverse])

    def solve(c, inverse, half):
        where_to, live = places(c)
        src, dst = xs.at[c % 2], ys
        pairs = [(m, n) for i, m in enumerate(tiles) for n in tiles[: i + 1]]
        for step in range(STEPS - 1):
            if step:
                src, dst = dst, src
            last = step == STEPS - 2
            for m, n in pairs:
                square = nn(src[m, :], src[:, n])
                if last:
                    value = square.astype(BF)
                    ms[m, n] = value
                    if m != n:
                        ms[n, m] = value.T
                else:
                    base = 1.5 * big if m == n else 0.0
                    ms[m, n] = (base - (half if step == 0 else 0.5) * square).astype(BF)
                yield
            if last:
                break
            for m, n in pairs:
                value = nn(src[m, n.start :], ms[n.start :, n])
                if n.start:
                    value = value + nt(src[m, : n.start], ms[n, : n.start])
                if step == 0:
                    value = value * inverse
                value = value.astype(BF)
                dst[m, n] = value
                if m != n:
                    dst[n, m] = value.T
                yield

        def times_m(v):
            return 1.5 * v - 0.5 * nn(v.astype(BF), ms[...])

        first_m = 1.5 * top - 0.5 * ms[:BS, :].astype(F32)
        square = nn(times_m(first_m).astype(BF), ms[...])
        yield
        after = times_m(1.5 * top - 0.5 * square)
        yield
        part = nn(after.astype(BF), src[...])
        part = (0.5 * (top + part)).astype(BF)
        for s in range(KMAX):
            place = jnp.where(live[s], where_to[s], SPAN)
            pb[rows(c), pl.ds(pl.multiple_of(place * BS, BS), BS)] = part[:, rows(s)]
            yield

    scales = []
    for _ in assemble(0, scales):
        pass
    for c in range(OWN + 1):
        following = []
        coming = assemble(c + 1, following) if c < OWN else iter(())
        for _ in solve(c, *scales):
            next(coming, None)
        for _ in coming:
            pass
        scales = following

    for j in range(OWN):
        rt[rows(j), :] = nn(zl[BACK + j + 1], pb[rows(j, 2), BS : SPAN * BS]).astype(BF)
    copies = []
    for i in range(SPAN):
        if i == 0:
            part = nt(zl[1, :, BS:], rt[:, rows(0)])
        elif i == SPAN - 1:
            part = nt(zl[i + 1, :, :BS], rt[:, rows(i - 1)])
        else:
            part = nt(zl[i + 1], rt[:, rows(i - 1, 2)])
        for j in range(OWN):
            if 0 <= i - j < 13:
                ob[j, i - j] = part[:, rows(j)]
                copy = pltpu.make_async_copy(
                    ob.at[j, i - j], out.at[j, i - j], sems.at[j * 13 + i - j]
                )
                copy.start()
                copies.append(copy)
    for copy in copies:
        copy.wait()


def scratch():
    return [
        pltpu.VMEM((SPAN, 4 * BS, 2 * BS), BF),
        pltpu.VMEM((SPAN, 2 * BS, BS), BF),
        pltpu.VMEM((SPAN + 1, BS, 2 * BS), BF),
        pltpu.VMEM((SPAN, BS, 4 * BS), BF),
        pltpu.VMEM((4 * SPAN, BS, BS), BF),
        pltpu.VMEM((2, ORDER, ORDER), BF),
        pltpu.VMEM((ORDER, ORDER), BF),
        pltpu.VMEM((ORDER, ORDER), BF),
        pltpu.VMEM((3 * BS, (SPAN + 1) * BS), BF),
        pltpu.VMEM((2 * BS, (SPAN - 1) * BS), BF),
        pltpu.VMEM((OWN, 13, BS, BS), F32),
        pltpu.SMEM((3 * KMAX,), jnp.int32),
        pltpu.SMEM((OWN, KMAX), jnp.int32),
        pltpu.SemaphoreType.DMA((OWN * 13,)),
    ]


def build(mesh, interpret=False):
    n = mesh.shape["space"] * mesh.shape["inner"]
    inside = lambda i: 0 <= i < n
    swap = [(i, i ^ 1) for i in range(n)]

    def chips(parity):
        pairs = []
        for i in range(n):
            chip = i >> 1
            other = chip + 1 if (chip & 1) == parity else chip - 1
            pairs.append((i, 2 * other + (i & 1)))
        return [(a, b) for a, b in pairs if inside(b)]

    cross = [(i, i + 3 if i & 1 else i - 3) for i in range(n)]
    cross = [(a, b) for a, b in cross if inside(b)]

    def send(value, pairs):
        return lax.ppermute(value, AXES, pairs)

    in_hbm = lambda x: x if interpret else pltpu.with_memory_space_constraint(x, pltpu.HBM)
    vmem = pl.BlockSpec(memory_space=pltpu.VMEM)
    anywhere = pl.BlockSpec(memory_space=pltpu.HBM)

    def local(hamiltonian, pattern, ortho, lists):
        pay, far = pl.pallas_call(
            pack_kernel,
            out_shape=(jax.ShapeDtypeStruct((PAY, BS), BF), jax.ShapeDtypeStruct((FAR, BS), BF)),
            in_specs=[anywhere] * 4,
            out_specs=(vmem, vmem),
            scratch_shapes=[
                pltpu.SMEM(pattern.shape, jnp.int32),
                pltpu.SMEM(lists.shape, jnp.int32),
                pltpu.VMEM((OWN, 3, BS, BS), BF),
                pltpu.VMEM((OWN, 2, BS, BS), BF),
                pltpu.SemaphoreType.DMA((OWN + 3,)),
            ],
            compiler_params=pltpu.CompilerParams(vmem_limit_bytes=8 << 20),
            interpret=interpret,
        )(in_hbm(pattern), in_hbm(lists), in_hbm(hamiltonian), in_hbm(ortho))
        near_b = send(pay, chips(1))
        near_a = send(pay, chips(0))
        got_far = send(far, cross)
        pair = send(pay, swap)
        cross_a = send(near_a, swap)
        cross_b = send(near_b, swap)
        out = pl.pallas_call(
            main_kernel,
            out_shape=jax.ShapeDtypeStruct((OWN, 13, BS, BS), F32),
            in_specs=[anywhere] + [vmem] * 7,
            out_specs=anywhere,
            scratch_shapes=scratch(),
            compiler_params=pltpu.CompilerParams(vmem_limit_bytes=24 << 20),
            cost_estimate=pl.CostEstimate(
                flops=12 * 10**9, bytes_accessed=4 << 20, transcendentals=0
            ),
            interpret=interpret,
        )(in_hbm(lists), pay, pair, near_a, near_b, cross_a, cross_b, got_far)
        return out

    spec4 = P(AXES, None, None, None)
    spec2 = P(AXES, None)
    return jax.shard_map(
        local, mesh=mesh, in_specs=(spec4, spec2, spec4, spec2), out_specs=spec4, check_vma=False
    )


def solution(mesh):
    return build(mesh)
```

```python
import functools

import jax
import jax.numpy as jnp
from jax import lax
from jax.experimental import pallas as pl
from jax.experimental.pallas import tpu as pltpu
from jax.sharding import PartitionSpec as P


AXES = ("space", "inner")
BS = 128
RO = 3
KMAX = 6
STEPS = 3
CHEM = 0.25
OWN = 2
SPAN = 14
BACK = 6
ORDER = KMAX * BS
PAY = 9 * BS + 16
FAR = 7 * BS + 16
TILE = 256


BF = jnp.bfloat16
F32 = jnp.float32


def nn(a, b):
    return jnp.dot(a, b, preferred_element_type=F32)


def nt(a, b):
    return lax.dot_general(a, b, (((1,), (1,)), ((), ())), preferred_element_type=F32)


def rows(i, n=1):
    return slice(i * BS, (i + n) * BS)


def eye(n, m):
    r = lax.broadcasted_iota(jnp.int32, (n, m), 0)
    c = lax.broadcasted_iota(jnp.int32, (n, m), 1)
    return jnp.where(r == c, 1.0, 0.0).astype(F32)


def position():
    device = lax.axis_index(AXES).astype(jnp.int32)
    return device * OWN, device & 1, (device >> 1) & 1


def pack_kernel(pattern, lists, ham, ortho, pay, far, keep, slot_of, hs, sems):
    first, core, _ = position()
    copies = [
        pltpu.make_async_copy(ham.at[c, pl.ds(2, 3)], hs.at[c], sems.at[c]) for c in range(OWN)
    ] + [
        pltpu.make_async_copy(pattern, keep, sems.at[OWN]),
        pltpu.make_async_copy(lists, slot_of, sems.at[OWN + 1]),
    ]
    places = [(pay, 5, 1, 0), (pay, 6, 1, 1), (pay, 7, 0, 0), (pay, 8, 0, 1), (far, 5, 1, 0), (far, 6, 1, 1)]
    straight = [
        pltpu.make_async_copy(ortho.at[j, k], to.at[pl.ds(i * BS, BS)], sems.at[OWN + 2 + n])
        for n, (to, i, j, k) in enumerate(places)
    ]
    for copy in copies + straight:
        copy.start()
    for copy in copies:
        copy.wait()

    r = lax.broadcasted_iota(jnp.int32, (BS, BS), 0)
    c = lax.broadcasted_iota(jnp.int32, (BS, BS), 1)
    masked = [
        [hs[j, k].astype(F32) * keep[j, k + 2].astype(F32) for k in range(3)]
        for j in range(OWN)
    ]
    pay[rows(0), :] = jnp.where(r >= c, masked[0][0], masked[1][0]).astype(BF)
    for j in range(OWN):
        for k in range(1, 3):
            pay[rows(2 * j + k), :] = masked[j][k].astype(BF)
    diagonal = jnp.sum(jnp.where(r == c, masked[1][0], 0.0), axis=0, keepdims=True)
    lane = lax.broadcasted_iota(jnp.int32, (16, BS), 1)
    row = lax.broadcasted_iota(jnp.int32, (16, BS), 0)
    extra = jnp.where(row == 1, diagonal, 0.0)
    for s in range(KMAX):
        slot = slot_of[0, s]
        value = jnp.where(slot >= 0, slot - first + BACK + 2, 0).astype(F32)
        extra = extra + jnp.where((lane == s) & (row == 0), value, 0.0)
    pay[PAY - 16 : PAY, :] = extra.astype(BF)

    far[rows(0, 5), :] = pay[rows(0, 5), :]
    far[FAR - 16 : FAR, :] = extra.astype(BF)
    for copy in straight:
        copy.wait()

    @pl.when(first == 0)
    def _():
        pay[rows(7), :] = jnp.zeros((BS, BS), BF)

    @pl.when(core == 0)
    def _():
        far[rows(2, 2), :] = pay[rows(7, 2), :]


def main_kernel(
    lists, own, pair, near_a, near_b, cross_a, cross_b, far, out,
    hb, zc, zl, gt, up, xs, ms, ys, pb, rt, ob, slots, slot_of, sems,
):
    first, core, odd_chip = position()
    lists_copy = pltpu.make_async_copy(lists, slot_of, sems.at[0])
    lists_copy.start()
    row_at = lax.broadcasted_iota(jnp.int32, (BS, BS), 0)
    lane_at = lax.broadcasted_iota(jnp.int32, (BS, BS), 1)
    ident = eye(BS, BS)

    def put_z(i, upper, diagonal):
        diag = (ident + diagonal.astype(F32)).astype(BF)
        zc[i, :BS, :] = upper
        zc[i, BS:, :] = diag
        zl[i, :, BS:] = upper
        zl[i + 1, :, :BS] = diag

    def put_h(i, k, block):
        hb[i, rows(k + 1), BS:] = block
        if i + 1 < SPAN:
            hb[i + 1, rows(k), :BS] = block
        if k == 1 and i + 1 < SPAN:
            hb[i + 1, rows(0), BS:] = block.T

    def take(k, pay, from_far=None):
        i = 2 * k + BACK
        size = PAY if from_far is None else FAR
        both = pay[rows(0), :].astype(F32)
        turned = pay[rows(0), :].T.astype(F32)
        last = pay[size - 16 : size, :].astype(F32)[1:2, :]
        put_h(i, 0, jnp.where(row_at >= lane_at, both, turned).astype(BF))
        diagonal = jnp.where(
            row_at < lane_at,
            both,
            jnp.where(row_at > lane_at, turned, jnp.broadcast_to(last, (BS, BS))),
        )
        put_h(i + 1, 0, diagonal.astype(BF))
        for j in range(OWN):
            for k in range(1, 3):
                put_h(i + j, k, pay[rows(2 * j + k), :])
        put_z(i + 1, pay[rows(5), :], pay[rows(6), :])
        if from_far is None:
            put_z(i, pay[rows(7), :], pay[rows(8), :])
        elif from_far == "right":
            put_z(i, pay[rows(2), :], pay[rows(3), :])

    def slots_of(pay):
        code = pay[PAY - 16 : PAY, :].astype(F32)
        lane = lax.broadcasted_iota(jnp.int32, (16, BS), 1)
        row = lax.broadcasted_iota(jnp.int32, (16, BS), 0)
        for s in range(KMAX):
            value = jnp.sum(jnp.where((lane == s) & (row == 0), code, 0.0)).astype(jnp.int32)
            slots[2 * KMAX + s] = jnp.where(value > 0, value, -1)

    take(0, own)

    def sides(near_l, cross_l, near_r, cross_r):
        @pl.when(core == 0)
        def _():
            take(-3, far, "left")
            take(-2, near_l)
            take(-1, cross_l)
            take(1, pair)
            take(2, near_r)
            take(3, cross_r)
            slots_of(pair)

        @pl.when(core == 1)
        def _():
            take(-3, cross_l)
            take(-2, near_l)
            take(-1, pair)
            take(1, cross_r)
            take(2, near_r)
            take(3, far, "right")
            slots_of(cross_r)

    @pl.when(odd_chip == 0)
    def _():
        sides(near_b, cross_b, near_a, cross_a)

    @pl.when(odd_chip == 1)
    def _():
        sides(near_a, cross_a, near_b, cross_b)

    for b in range(1, SPAN):
        hb[b, rows(3), :BS] = jnp.zeros((BS, BS), BF)
        gt[b] = nt(zc[b].T, hb[b]).astype(BF)
    for b in range(1, SPAN):
        for k in range(RO + 1):
            if b + k < SPAN:
                if k < RO:
                    block = nn(gt[b, :, rows(k, 2)], zc[b + k])
                else:
                    block = nn(gt[b, :, rows(k)], zc[b + k, :BS, :])
                up[4 * b + k] = (-block).astype(BF)

    lists_copy.wait()
    for j in range(OWN):
        for s in range(KMAX):
            slot = slot_of[j, s]
            slots[j * KMAX + s] = jnp.where(slot >= 0, slot - first + BACK, -1)
    pb[...] = jnp.zeros_like(pb)

    tiles = [slice(i * TILE, (i + 1) * TILE) for i in range(ORDER // TILE)]
    big = eye(TILE, TILE)
    top = eye(BS, ORDER)

    def places(c):
        where_to = [slots[c * KMAX + s] for s in range(KMAX)]
        return where_to, [w >= 0 for w in where_to]

    def assemble(c, result):
        where_to, live = places(c)
        count = functools.reduce(lambda a, b: a + b, [v.astype(jnp.int32) for v in live])
        squares = jnp.zeros((BS, BS), F32)
        x = xs.at[c % 2]
        for s in range(KMAX):
            block = up[jnp.where(live[s], 4 * where_to[s], 0)].astype(F32)
            entry = jnp.where(live[s], CHEM * ident + block, 0.0)
            squares = squares + entry * entry
            x[rows(s), rows(s)] = entry.astype(BF)
            yield
            for t in range(s):
                ws, wt = where_to[s], where_to[t]
                lo, hi = jnp.minimum(ws, wt), jnp.maximum(ws, wt)
                valid = live[s] & live[t] & (hi - lo <= RO)
                block = up[jnp.where(valid, 4 * lo + (hi - lo), 0)]
                turned = block.T
                block = jnp.where(valid, block, jnp.zeros_like(block))
                turned = jnp.where(valid, turned, jnp.zeros_like(turned))
                x[rows(s), rows(t)] = jnp.where(ws >= wt, turned, block)
                x[rows(t), rows(s)] = jnp.where(ws >= wt, block, turned)
                wide = block.astype(F32)
                squares = squares + 2.0 * (wide * wide)
                yield
        total = jnp.sum(squares, axis=(0, 1), keepdims=True)
        width = (jnp.maximum(count, 1) * BS).astype(F32)
        inverse = 1.0 / (2.0 * jnp.sqrt(total / width + 1e-06))
        result.extend([inverse, 0.5 * inverse * inverse])

    def solve(c, inverse, half):
        where_to, live = places(c)
        src, dst = xs.at[c % 2], ys
        pairs = [(m, n) for i, m in enumerate(tiles) for n in tiles[: i + 1]]
        for step in range(STEPS - 1):
            if step:
                src, dst = dst, src
            last = step == STEPS - 2
            for m, n in pairs:
                square = nn(src[m, :], src[:, n])
                if last:
                    value = square.astype(BF)
                    ms[m, n] = value
                    if m != n:
                        ms[n, m] = value.T
                else:
                    base = 1.5 * big if m == n else 0.0
                    ms[m, n] = (base - (half if step == 0 else 0.5) * square).astype(BF)
                yield
            if last:
                break
            for m, n in pairs:
                value = nn(src[m, n.start :], ms[n.start :, n])
                if n.start:
                    value = value + nt(src[m, : n.start], ms[n, : n.start])
                if step == 0:
                    value = value * inverse
                value = value.astype(BF)
                dst[m, n] = value
                if m != n:
                    dst[n, m] = value.T
                yield

        def times_m(v):
            return 1.5 * v - 0.5 * nn(v.astype(BF), ms[...])

        first_m = 1.5 * top - 0.5 * ms[:BS, :].astype(F32)
        square = nn(times_m(first_m).astype(BF), ms[...])
        yield
        after = times_m(1.5 * top - 0.5 * square)
        yield
        part = nn(after.astype(BF), src[...])
        part = (0.5 * (top + part)).astype(BF)
        for s in range(KMAX):
            place = jnp.where(live[s], where_to[s], SPAN)
            pb[rows(c), pl.ds(pl.multiple_of(place * BS, BS), BS)] = part[:, rows(s)]
            yield

    scales = []
    for _ in assemble(0, scales):
        pass
    for c in range(OWN + 1):
        following = []
        coming = assemble(c + 1, following) if c < OWN else iter(())
        for _ in solve(c, *scales):
            next(coming, None)
        for _ in coming:
            pass
        scales = following

    for j in range(OWN):
        rt[rows(j), :] = nn(zl[BACK + j + 1], pb[rows(j, 2), BS : SPAN * BS]).astype(BF)
    copies = []
    for i in range(SPAN):
        if i == 0:
            part = nt(zl[1, :, BS:], rt[:, rows(0)])
        elif i == SPAN - 1:
            part = nt(zl[i + 1, :, :BS], rt[:, rows(i - 1)])
        else:
            part = nt(zl[i + 1], rt[:, rows(i - 1, 2)])
        for j in range(OWN):
            if 0 <= i - j < 13:
                ob[j, i - j] = part[:, rows(j)]
                copy = pltpu.make_async_copy(
                    ob.at[j, i - j], out.at[j, i - j], sems.at[j * 13 + i - j]
                )
                copy.start()
                copies.append(copy)
    for copy in copies:
        copy.wait()


def scratch():
    return [
        pltpu.VMEM((SPAN, 4 * BS, 2 * BS), BF),
        pltpu.VMEM((SPAN, 2 * BS, BS), BF),
        pltpu.VMEM((SPAN + 1, BS, 2 * BS), BF),
        pltpu.VMEM((SPAN, BS, 4 * BS), BF),
        pltpu.VMEM((4 * SPAN, BS, BS), BF),
        pltpu.VMEM((2, ORDER, ORDER), BF),
        pltpu.VMEM((ORDER, ORDER), BF),
        pltpu.VMEM((ORDER, ORDER), BF),
        pltpu.VMEM((3 * BS, (SPAN + 1) * BS), BF),
        pltpu.VMEM((2 * BS, (SPAN - 1) * BS), BF),
        pltpu.VMEM((OWN, 13, BS, BS), F32),
        pltpu.SMEM((3 * KMAX,), jnp.int32),
        pltpu.SMEM((OWN, KMAX), jnp.int32),
        pltpu.SemaphoreType.DMA((OWN * 13,)),
    ]


def build(mesh, interpret=False):
    n = mesh.shape["space"] * mesh.shape["inner"]
    inside = lambda i: 0 <= i < n
    swap = [(i, i ^ 1) for i in range(n)]

    def chips(parity):
        pairs = []
        for i in range(n):
            chip = i >> 1
            other = chip + 1 if (chip & 1) == parity else chip - 1
            pairs.append((i, 2 * other + (i & 1)))
        return [(a, b) for a, b in pairs if inside(b)]

    cross = [(i, i + 3 if i & 1 else i - 3) for i in range(n)]
    cross = [(a, b) for a, b in cross if inside(b)]

    def send(value, pairs):
        return lax.ppermute(value, AXES, pairs)

    in_hbm = lambda x: x if interpret else pltpu.with_memory_space_constraint(x, pltpu.HBM)
    vmem = pl.BlockSpec(memory_space=pltpu.VMEM)
    anywhere = pl.BlockSpec(memory_space=pltpu.HBM)

    def local(hamiltonian, pattern, ortho, lists):
        pay, far = pl.pallas_call(
            pack_kernel,
            out_shape=(jax.ShapeDtypeStruct((PAY, BS), BF), jax.ShapeDtypeStruct((FAR, BS), BF)),
            in_specs=[anywhere] * 4,
            out_specs=(vmem, vmem),
            scratch_shapes=[
                pltpu.SMEM(pattern.shape, jnp.int32),
                pltpu.SMEM(lists.shape, jnp.int32),
                pltpu.VMEM((OWN, 3, BS, BS), BF),
                pltpu.SemaphoreType.DMA((OWN + 8,)),
            ],
            compiler_params=pltpu.CompilerParams(vmem_limit_bytes=8 << 20),
            interpret=interpret,
        )(in_hbm(pattern), in_hbm(lists), in_hbm(hamiltonian), in_hbm(ortho))
        near_b = send(pay, chips(1))
        near_a = send(pay, chips(0))
        got_far = send(far, cross)
        pair = send(pay, swap)
        cross_a = send(near_a, swap)
        cross_b = send(near_b, swap)
        out = pl.pallas_call(
            main_kernel,
            out_shape=jax.ShapeDtypeStruct((OWN, 13, BS, BS), F32),
            in_specs=[anywhere] + [vmem] * 7,
            out_specs=anywhere,
            scratch_shapes=scratch(),
            compiler_params=pltpu.CompilerParams(vmem_limit_bytes=24 << 20),
            cost_estimate=pl.CostEstimate(
                flops=12 * 10**9, bytes_accessed=4 << 20, transcendentals=0
            ),
            interpret=interpret,
        )(in_hbm(lists), pay, pair, near_a, near_b, cross_a, cross_b, got_far)
        return out

    spec4 = P(AXES, None, None, None)
    spec2 = P(AXES, None)
    return jax.shard_map(
        local, mesh=mesh, in_specs=(spec4, spec2, spec4, spec2), out_specs=spec4, check_vma=False
    )


def solution(mesh):
    return build(mesh)
```
